32 devices in a mesh: batch: 2 (over x), sy: 4 (over z), sx: 4 (over y, core).
Axes of the slice: x: 2, y: 2, z: 4, core: 2. Of those that a mesh axis runs over, the one named last changes fastest.
Arguments:
- forcing: float32 [256, 128, 256], P(('batch', 'sx'), 'sy'), parts along dimension 0
- kappa: float32 [256, 128], P(('batch', 'sx'), 'sy'), parts along dimension 0
- local_inv: float32 [32, 1600, 1600], P(('batch', 'sx', 'sy')), parts along dimension 0
- coarse_basis: float32 [32, 1024, 8], P(('batch', 'sx', 'sy')), parts along dimension 0
- coarse_counts: int32 [32], P(('batch', 'sx', 'sy')), parts along dimension 0
- coarse_inv: float32 [128, 64], P('batch'), parts along dimension 0
Outputs:
- output 1: float32 [256, 128, 256], P(('batch', 'sx'), 'sy'), parts along dimension 0
- output 2: float32 [16, 256], P('batch'), parts along dimension 0
There are 2 independent parts. The reference program is written for one: setup_inputs(seed, part) draws one part's arguments, and reference() takes and returns one part's arrays. A program takes and returns all parts, laid end to end along the dimension named above; each array names one.
All inputs are finite; a program needn't handle non-finite values.
Results may differ from the reference program's by a relative error of at most 0.001.
Values are sent between devices in bfloat16 or wider.
A program may use at most 1 GiB of HBM per device.

```python
import jax
import jax.numpy as jnp
from jax import lax

SX = 4
SY = 4
M = 32
D = 4
KMAX = 8
B = 256
ITERS = 8
ME = M + D + D
NE = ME * ME
NPART = SX * SY
KTOT = NPART * KMAX // 2
CONTRAST = 1000.0


def edge_weights(kappa):
    kappa_pad = jnp.pad(kappa, 1, mode='edge')
    middle = kappa_pad[1:-1, 1:-1]

    def harmonic(other):
        return 2.0 * middle * other / (middle + other)
    return (harmonic(kappa_pad[:-2, 1:-1]), harmonic(kappa_pad[2:, 1:-1]), harmonic(kappa_pad[1:-1, :-2]), harmonic(kappa_pad[1:-1, 2:]))


def apply_op(weights, field):
    w_north, w_south, w_west, w_east = weights
    diagonal = w_north + w_south + w_west + w_east
    field_pad = jnp.pad(field, ((1, 1), (1, 1), (0, 0)))
    return (diagonal[:, :, None] * field - w_north[:, :, None] * field_pad[:-2, 1:-1] - w_south[:, :, None] * field_pad[2:, 1:-1] - w_west[:, :, None] * field_pad[1:-1, :-2] - w_east[:, :, None] * field_pad[1:-1, 2:])


def to_blocks(field):
    return field.reshape(SX, M, SY, M, -1).transpose(0, 2, 1, 3, 4).reshape(NPART, M * M, -1)


def from_blocks(blocks):
    return blocks.reshape(SX, SY, M, M, -1).transpose(0, 2, 1, 3, 4).reshape(SX * M, SY * M, -1)


def extend_blocks(field):
    rows = field.reshape(SX, M, SY * M, -1)
    zero_rows = jnp.zeros_like(rows[:1, :D])
    top = jnp.concatenate([zero_rows, rows[:-1, M - D:]], axis=0)
    bottom = jnp.concatenate([rows[1:, :D], zero_rows], axis=0)
    rows = jnp.concatenate([top, rows, bottom], axis=1)
    columns = rows.reshape(SX, ME, SY, M, -1)
    zero_cols = jnp.zeros_like(columns[:, :, :1, :D])
    left = jnp.concatenate([zero_cols, columns[:, :, :-1, M - D:]], axis=2)
    right = jnp.concatenate([columns[:, :, 1:, :D], zero_cols], axis=2)
    columns = jnp.concatenate([left, columns, right], axis=3)
    return columns.transpose(0, 2, 1, 3, 4)


def fold_blocks(extended):
    columns = extended.transpose(0, 2, 1, 3, 4)
    left = columns[:, :, :, :D]
    right = columns[:, :, :, M + D:]
    zero_cols = jnp.zeros_like(left[:, :, :1])
    from_right = jnp.concatenate([left[:, :, 1:], zero_cols], axis=2)
    from_left = jnp.concatenate([zero_cols, right[:, :, :-1]], axis=2)
    center = (columns[:, :, :, D:D + M] + jnp.pad(from_right, ((0, 0), (0, 0), (0, 0), (M - D, 0), (0, 0))) + jnp.pad(from_left, ((0, 0), (0, 0), (0, 0), (0, M - D), (0, 0))))
    rows = center.reshape(SX, ME, SY * M, -1)
    top = rows[:, :D]
    bottom = rows[:, M + D:]
    zero_rows = jnp.zeros_like(top[:1])
    from_below = jnp.concatenate([top[1:], zero_rows], axis=0)
    from_above = jnp.concatenate([zero_rows, bottom[:-1]], axis=0)
    center = (rows[:, D:D + M] + jnp.pad(from_below, ((0, 0), (M - D, 0), (0, 0), (0, 0))) + jnp.pad(from_above, ((0, 0), (0, M - D), (0, 0), (0, 0))))
    return center.reshape(SX * M, SY * M, -1)


def pack_order(counts):
    slot = jnp.arange(NPART * KMAX)
    valid = (slot % KMAX) < counts[slot // KMAX]
    order = jnp.argsort(jnp.where(valid, 0, 1) * (NPART * KMAX) + slot)
    return order[:KTOT]


def draw_counts(key):
    key_perm, key_shift = jax.random.split(key)
    order = jax.random.permutation(key_perm, NPART)
    shift = jax.random.randint(key_shift, (NPART // 2,), 0, KMAX // 2)
    shift = shift.at[0].set(KMAX // 2 - 1)
    counts = jnp.full((NPART,), KMAX // 2, jnp.int32)
    counts = counts.at[order[0::2]].add(shift).at[order[1::2]].add(-shift)
    return counts.astype(jnp.int32)


def build_basis(amplitude, counts):
    column = jnp.arange(KMAX)
    freq_row = (column + 1) // 2
    freq_col = column // 2
    grid = (jnp.arange(M) + 0.5) * (jnp.pi / M)
    wave_row = jnp.cos(grid[:, None] * freq_row[None, :])
    wave_col = jnp.cos(grid[:, None] * freq_col[None, :])
    modes = (wave_row[:, None, :] * wave_col[None, :, :]).reshape(M * M, KMAX)
    keep = (column[None, :] < counts[:, None]).astype(jnp.float32) * amplitude
    return modes[None, :, :] * keep[:, None, :]


def build_inverses(kappa, basis, counts):
    weights = edge_weights(kappa)
    w_north, w_south, w_west, w_east = weights
    diagonal = w_north + w_south + w_west + w_east
    east_in = w_east * (jnp.arange(SY * M) < SY * M - 1)[None, :]
    south_in = w_south * (jnp.arange(SX * M) < SX * M - 1)[:, None]
    diag_ext = extend_blocks(diagonal[:, :, None] - 1.0).reshape(NPART, ME, ME) + 1.0
    east_ext = extend_blocks(east_in[:, :, None]).reshape(NPART, ME, ME) * (jnp.arange(ME) < ME - 1)[None, None, :]
    south_ext = extend_blocks(south_in[:, :, None]).reshape(NPART, ME, ME) * (jnp.arange(ME) < ME - 1)[None, :, None]

    def local_matrix(pieces):
        diag_block, east_block, south_block = pieces
        east_flat = east_block.reshape(-1)[:-1]
        south_flat = south_block.reshape(-1)[:-ME]
        matrix = jnp.diag(diag_block.reshape(-1)) - jnp.diag(east_flat, 1) - jnp.diag(east_flat, -1) - jnp.diag(south_flat, ME) - jnp.diag(south_flat, -ME)
        return jnp.linalg.inv(matrix)
    local_inv = lax.map(local_matrix, (diag_ext, east_ext, south_ext))
    local_inv = 0.5 * (local_inv + jnp.swapaxes(local_inv, 1, 2))

    def coarse_row(index):
        single = basis * (jnp.arange(NPART) == index)[:, None, None]
        image = apply_op(weights, from_blocks(single))
        return jnp.einsum('smk,smc->skc', basis, to_blocks(image)).reshape(NPART * KMAX, KMAX)
    stacked = lax.map(coarse_row, jnp.arange(NPART))
    full = jnp.transpose(stacked, (1, 0, 2)).reshape(NPART * KMAX, NPART * KMAX)
    packed = pack_order(counts)
    coarse = full[packed][:, packed]
    coarse_inv = jnp.linalg.inv(coarse)
    coarse_inv = 0.5 * (coarse_inv + coarse_inv.T)
    return local_inv, coarse_inv


def setup_inputs(seed: int = 0, part: int = 0) -> dict:
    key = jax.random.fold_in(jax.random.key(seed), part)
    keys = jax.random.split(key, 6)
    base = jnp.exp(0.5 * jax.random.normal(keys[0], (SX * M, SY * M), jnp.float32))
    row_channel = jax.random.randint(keys[1], (SX * M,), 0, 6) == 0
    col_channel = jax.random.randint(keys[2], (SY * M,), 0, 6) == 0
    kappa = base * jnp.where(row_channel[:, None] | col_channel[None, :], CONTRAST, 1.0)
    counts = draw_counts(keys[3])
    forcing = jax.random.normal(keys[4], (SX * M, SY * M, B), jnp.float32)
    amplitude = jax.random.uniform(keys[5], (NPART, KMAX), jnp.float32, 0.5, 1.5)
    basis = build_basis(amplitude, counts)
    local_inv, coarse_inv = build_inverses(kappa, basis, counts)
    return {'forcing': forcing, 'kappa': kappa, 'local_inv': local_inv, 'coarse_basis': basis, 'coarse_counts': counts, 'coarse_inv': coarse_inv}


def reference(forcing, kappa, local_inv, coarse_basis, coarse_counts, coarse_inv):
    weights = edge_weights(kappa)
    packed = pack_order(coarse_counts)

    def col_dot(first, second):
        return jnp.sum(first * second, axis=(0, 1))

    def precondition(resid):
        extended = extend_blocks(resid).reshape(NPART, NE, B)
        local = jnp.einsum('sij,sjb->sib', local_inv.astype(jnp.float32), extended)
        level_one = fold_blocks(local.reshape(SX, SY, ME, ME, B))
        restrict = jnp.einsum('smk,smb->skb', coarse_basis, to_blocks(resid)).reshape(NPART * KMAX, B)
        coarse = jnp.dot(coarse_inv, restrict[packed])
        spread = jnp.zeros((NPART * KMAX, B), jnp.float32).at[packed].set(coarse)
        level_two = from_blocks(jnp.einsum('smk,skb->smb', coarse_basis, spread.reshape(NPART, KMAX, B)))
        return level_one + level_two

    forcing_norm = jnp.sqrt(col_dot(forcing, forcing))
    solution = jnp.zeros_like(forcing)
    resid = forcing
    precond = precondition(resid)
    direction = precond
    rz_dot = col_dot(resid, precond)
    norms = []
    for step in range(ITERS):
        image = apply_op(weights, direction)
        alpha = rz_dot / col_dot(direction, image)
        solution = solution + alpha * direction
        resid = resid - alpha * image
        norms.append(jnp.sqrt(col_dot(resid, resid)) / forcing_norm)
        if step < ITERS - 1:
            precond = precondition(resid)
            rz_new = col_dot(resid, precond)
            direction = precond + (rz_new / rz_dot) * direction
            rz_dot = rz_new
    return solution, jnp.stack(norms)
```

```python
import jax
import jax.numpy as jnp
from jax import lax
from jax.experimental import pallas as pl
from jax.experimental.pallas import tpu as pltpu
from jax.sharding import PartitionSpec as P

ITERS = 8
M = 32
D = 4
ME = M + 2 * D
NE = ME * ME
SUB = 8
LANES = 128
TILE = 256
KT = NE // TILE
KM = KT * TILE
REM = NE - KM
ROWS = 10
CHUNK = ROWS * ME
BT = 16
NL = NE + 2 * BT
KMAX = 8
GRID = 128
LOW = M + SUB + D
WIDE = M + 2 * SUB
OWN = D + 1
STRIP = 9
EDGE = STRIP + 2
MESH = pl.DeviceIdType.MESH
HI = lax.Precision.HIGHEST
F32 = jnp.float32
BF16 = jnp.bfloat16
HALVES = (0, 1)
PIECES = (0, 1, 2)
FAR = (1, 2, 3)
LAST = FAR[-1]
SIDE = FAR[-1] + 1


def lanes(h):
    return slice(LANES * h, LANES * (h + 1))


def tile(k):
    return slice(TILE * k, TILE * (k + 1))


def mult(v, n=BT):
    return v if isinstance(v, int) else pl.multiple_of(v, n)


def row(v, k):
    return v[k:k + 1]


def wide(v):
    return jnp.broadcast_to(v, (SUB, LANES))


def colsum(v):
    return jnp.sum(v, axis=0, keepdims=True)


def each(copies, what):
    for c in copies:
        getattr(c, what)()


def split3(v):
    hi = v.astype(BF16)
    rest = v - hi.astype(F32)
    mid = rest.astype(BF16)
    low = (rest - mid.astype(F32)).astype(BF16)
    return hi, mid, low


def solve_kernel(f_hbm, aux_hbm, inv_hbm, bt_ref, cinv_ref, cnt_ref, x_hbm, nrm_ref,
                 S48, L, Lr, stage, X, Xr, T, TE, z, p, r, l, x, Q, Ey, W5, Ecat, RE,
               V, HB, HE, HP, PK, G1a, G2a, G1b, G2b, G1d, G2d, Ccat, cr, wr, cst, pqs,
               ld_sem, own_sem, h0_s, h0_r, v0_s, v0_r, v_s, v_r, hm_s, hm_r,
               a1_s, a1_r, a2_s, a2_r, b1_s, b1_r, b2_s, b2_r, d1_s, d1_r, d2_s, d2_r, out_sem):
    sx = lax.axis_index("sx")
    sy = lax.axis_index("sy")
    left, right = {"sy": sy - 1}, {"sy": sy + 1}
    has_left, has_right = sy > 0, sy < LAST
    has = (sx > 0, sx < LAST)
    near = lax.rem(sx, 2)
    inner = (sx > 0) & (sx < LAST)

    def rc(src, dst, s, q, dev):
        return pltpu.make_async_remote_copy(src, dst, s, q, device_id=dev, device_id_type=MESH)

    own = pl.ds(OWN, M)
    inv_cp = [pltpu.make_async_copy(inv_hbm.at[pl.ds(CHUNK * c, CHUNK)], stage.at[c], ld_sem.at[c]) for c in range(SIDE)]
    own_cp = [pltpu.make_async_copy(f_hbm.at[:, :, pl.ds(LANES * h, LANES)], S48.at[h, own, pl.ds(SUB, M)], own_sem.at[h]) for h in HALVES]
    own_cp += [pltpu.make_async_copy(aux_hbm.at[h], S48.at[2 + h, own, pl.ds(SUB, M)], own_sem.at[2 + h]) for h in HALVES]
    each(own_cp, "start")
    each(inv_cp, "start")
    zrow = jnp.zeros((SIDE, OWN, WIDE, LANES), F32)
    S48[:, 0:OWN] = zrow
    S48[:, OWN + M:] = zrow
    zcol = jnp.zeros((SIDE, M, SUB, LANES), F32)
    S48[:, OWN:OWN + M, 0:SUB] = zcol
    S48[:, OWN:OWN + M, ME:] = zcol
    for b in (V, HB, HE, HP):
        b[...] = jnp.zeros(b.shape, F32)

    bar = pltpu.get_barrier_semaphore()
    for d in FAR:
        pl.semaphore_signal(bar, inc=1, device_id={"sx": lax.rem(sx + d, SIDE)}, device_id_type=MESH)
        pl.semaphore_signal(bar, inc=1, device_id={"sy": lax.rem(sy + d, SIDE)}, device_id_type=MESH)
    pl.semaphore_wait(bar, 2 * LAST)

    def first_copies(G1, s, q):
        return [rc(G1.at[sy], G1.at[sy], s.at[d - 1], q.at[d - 1], {"sy": lax.rem(sy + d, SIDE)}) for d in FAR]

    def second_copies(src, G2, s, q):
        return [rc(src, G2.at[sx], s.at[d - 1], q.at[d - 1], {"sx": lax.rem(sx + d, SIDE)}) for d in FAR]

    a1 = first_copies(G1a, a1_s, a1_r)
    a2 = second_copies(G1a, G2a, a2_s, a2_r)
    b1 = first_copies(G1b, b1_s, b1_r)
    b2 = second_copies(G2b.at[sx], G2b, b2_s, b2_r)
    d1 = first_copies(G1d, d1_s, d1_r)
    d2 = second_copies(G2d.at[sx], G2d, d2_s, d2_r)
    mine_y, mine_x = pl.ds(sy, 1), pl.ds(sx, 1)

    def half_sum(G1, G2, one, two):
        each(one, "wait")
        G2[mine_x] = jnp.sum(G1[...], axis=0, keepdims=True)
        each(two, "start")

    def full_sum(G2, two):
        each(two, "wait")
        return jnp.sum(G2[...], axis=0)

    G1b[mine_y] = jnp.broadcast_to(cnt_ref[...], (1, 2, SUB, LANES))
    each(b1, "start")

    each(own_cp, "wait")
    h0l = rc(S48.at[:, own, pl.ds(SUB, SUB)], S48.at[:, own, pl.ds(ME, SUB)], h0_s.at[0], h0_r.at[0], left)
    h0r = rc(S48.at[:, own, pl.ds(M, SUB)], S48.at[:, own, pl.ds(0, SUB)], h0_s.at[1], h0_r.at[1], right)
    v0 = [rc(S48.at[:, pl.ds(OWN, OWN)], S48.at[:, pl.ds(OWN + M, OWN)], v0_s.at[0], v0_r.at[1], {"sx": sx - 1}),
          rc(S48.at[:, pl.ds(M, OWN)], S48.at[:, pl.ds(0, OWN)], v0_s.at[1], v0_r.at[0], {"sx": sx + 1})]
    v0_in = [rc(S48.at[:, pl.ds(0, OWN)], S48.at[:, pl.ds(0, OWN)], v0_s.at[e], v0_r.at[e], left) for e in HALVES]
    pl.when(has_left)(h0l.start)
    pl.when(has_right)(h0r.start)

    for b in (p, z, r, l, x, T):
        def zero(i, c, b=b):
            b[:, pl.ds(i, 1)] = jnp.zeros((2, 1, ME, LANES), F32)
            return c
        lax.fori_loop(0, b.shape[1], zero, 0)
    Xr[...] = jnp.zeros(Xr.shape, BF16)
    for b in (cr, wr, cst, pqs, nrm_ref):
        b[...] = jnp.zeros(b.shape, F32)

    def put_l(v, rows):
        one, two, three = split3(v)
        rest = []
        for k, piece in enumerate((one, two, three)):
            L[rows, KM * k:KM * (k + 1)] = piece[:, 0:KM]
            rest.append(piece[:, KM:].astype(F32))
        twice = jnp.concatenate(rest[0:2], axis=1).astype(BF16)
        Lr[rows, lanes(0)] = twice
        Lr[rows, lanes(1)] = twice
        Lr[rows, lanes(2)] = jnp.concatenate([rest[0], rest[2]], axis=1).astype(BF16)
        Lr[rows, lanes(LAST)] = jnp.zeros(twice.shape, BF16)

    for at in (0, LAST * CHUNK + BT):
        put_l(bt_ref[...], pl.ds(at, BT))
    half_sum(G1b, G2b, b1, b2)

    def split_inv(c):
        inv_cp[c].wait()

        def body(k, carry):
            put_l(stage[c, pl.ds(mult(BT * k), BT), :], pl.ds(mult(CHUNK * c + BT * (c // LAST + 1) + BT * k), BT))
            return carry
        lax.fori_loop(0, CHUNK // BT, body, 0)

    split_inv(0)
    split_inv(1)
    pl.when(has_left)(h0l.wait_send)
    pl.when(has_right)(h0r.wait_send)
    pl.when(has_right)(h0l.wait_recv)
    pl.when(has_left)(h0r.wait_recv)
    for e in HALVES:
        pl.when(has[e])(v0[e].start)
    split_inv(2)
    split_inv(LAST)

    def dot(a, b):
        return jnp.dot(a, b, preferred_element_type=F32)

    def dot_pieces(lhs, v):
        y1, y2, y3 = split3(v)
        total = 0.0
        for n, two in enumerate(((y1, y1), (y2, y2), (y3, y1))):
            total = total + dot(lhs(LANES * (n // 2)), jnp.concatenate(two, axis=0))
        return total

    cnt = full_sum(G2b, b2)[0]
    lane = lax.broadcasted_iota(jnp.int32, (SUB, LANES), 1)
    starts = cnt
    for d in (KMAX, 2 * KMAX, D * KMAX, SUB * KMAX):
        starts = starts + jnp.where(lane >= d, pltpu.roll(starts, d, 1), 0.0)
    starts = starts - cnt
    col = (lane % KMAX).astype(F32)
    target = jnp.where(col < cnt, starts + col, -1.0)
    half = cinv_ref.shape[0]
    pick = jnp.where(lax.broadcasted_iota(jnp.int32, (half, LANES), 0).astype(F32) == row(target, 0), 1.0, 0.0)

    def rhs_of(parts):
        v = jnp.concatenate(parts + [jnp.zeros_like(parts[0])], axis=0)
        return v.astype(BF16)

    def lhs_of(parts):
        v = jnp.concatenate(parts + [jnp.zeros_like(parts[0])], axis=1)
        return v.astype(BF16)

    def as_f32(v):
        return [piece.astype(F32) for piece in split3(v)]
    spread = dot(lhs_of(as_f32(cinv_ref[...])), rhs_of([pick] * len(PIECES)))
    spread = dot(lhs_of([pick.T] * len(PIECES)), rhs_of(as_f32(spread)))

    def put_middle(ref, rows, v):
        for k, piece in zip((1, 0, 2), split3(v)):
            ref[rows, lanes(k)] = piece
    put_middle(Ccat, pl.ds(0, LANES), spread)

    for e in HALVES:
        pl.when(has[e])(v0[e].wait_send)
        pl.when(has[e])(v0_in[e].wait_recv)

    jcol = lax.broadcasted_iota(jnp.int32, (ME, LANES), 0)
    gj = sy * M + jcol - D
    in_col = (gj >= 0) & (gj < GRID)

    def shifted(v, k=D):
        return pltpu.roll(v, WIDE - k, 0)[0:ME]

    def weights(i, c):
        gi = sx * M + i - D
        ok = in_col & (gi >= 0) & (gi < GRID)
        here = S48[LAST, i + 1]
        kc = shifted(here)

        def pair(other, inside):
            both = ok & inside
            w = jnp.where(both, 2.0 * kc * other / jnp.where(both, kc + other, 1.0), 0.0)
            return w, jnp.where(ok & jnp.logical_not(inside), kc, w)
        edges = (pair(shifted(S48[LAST, i]), ok & (gi > 0)), pair(shifted(S48[LAST, i + 2]), ok & (gi < GRID - 1)),
                 pair(shifted(here, D - 1), gj > 0), pair(shifted(here, D + 1), gj < GRID - 1))
        total = 0.0
        for k, (w, d) in enumerate(edges):
            W5[k, i] = w
            total = total + d
        W5[SIDE, i] = total
        return c
    lax.fori_loop(0, ME, weights, 0)

    for i in range(ME):
        RE[0, i:i + 1] = S48[2, i + 1, D - 1:D]
        RE[1, i:i + 1] = S48[2, i + 1, LOW:LOW + 1]

    def pair_of(two, k):
        return jnp.concatenate(two, axis=0), pl.ds(mult(2 * ME * k), 2 * ME)

    def basis_rows(k, c):
        v, rows = pair_of([shifted(S48[2, 2 * k]), shifted(S48[2, 2 * k + 1])], k)
        put_middle(Ecat, rows, v)
        return c
    lax.fori_loop(0, LOW // 2 - 1, basis_rows, 0)
    v, rows = pair_of([RE[0], RE[1]], LOW // 2 - 1)
    put_middle(Ecat, rows, v)

    def put_x(two, h, k):
        v, rows = pair_of(two, k)
        pieces = split3(v)
        if isinstance(k, int) and k == ME // 2 - 1:
            n = KM - 2 * ME * k
            for j, piece in enumerate(pieces):
                X[j, KM - n:KM, lanes(h)] = piece[0:n]
            for slot, j in enumerate((0, 0, 1, 1, 2, 0)):
                Xr[REM * slot:REM * (slot + 1), lanes(h)] = pieces[j][n:]
        else:
            for j, piece in enumerate(pieces):
                X[j, rows, lanes(h)] = piece

    def first_rows(k, c):
        for h in HALVES:
            two = [shifted(S48[h, 2 * k + 1 + j]) for j in HALVES]
            for j in HALVES:
                Q[h, 2 * k + 1 + j] = two[j]
            put_x(two, h, k)
        return c
    lax.fori_loop(0, ME // 2 - 1, first_rows, 0)
    first_rows(ME // 2 - 1, 0)

    colf = jnp.where((jcol >= D) & (jcol < D + M), 1.0, 0.0)
    sub8 = lax.broadcasted_iota(jnp.int32, (SUB, LANES), 0)
    zero = jnp.zeros((ME, LANES), F32)

    def product(start, n):
        rows = pl.ds(mult(start), n)
        total = dot(Lr[rows, :], Xr[...])
        for j in PIECES:
            for i in PIECES[:len(PIECES) - j]:
                total = total + dot(L[rows, KM * i:KM * (i + 1)], X[j])
        return total

    def put_t(out, c):
        for h in HALVES:
            T[h, pl.ds(1 + ROWS * c, ROWS)] = out[:, lanes(h)].reshape(ROWS, ME, LANES)

    def v_copy(e):
        return rc(T.at[:, pl.ds(1 + (M - 1) * e, STRIP)], V.at[1 - e], v_s.at[e], v_r.at[1 - e], {"sx": sx - 1 + 2 * e})

    def step(m, carry):
        par = lax.rem(m, 2)

        def side(n, src, dst):
            return [rc(src[j], dst.at[par, 1 - j], hm_s.at[par, j, n], hm_r.at[par, 1 - j, n], (left, right)[j]) for j in HALVES]

        def go(pair):
            pl.when(has_left)(pair[0].start)
            pl.when(has_right)(pair[1].start)

        def cols(ref, lo, n):
            return [ref.at[:, pl.ds(lo, n), pl.ds(M * j, SUB)] for j in HALVES]

        mids = [side(n, cols(T, EDGE + ROWS * n, ROWS), HB.at[:, :, n]) for n in HALVES]
        edges = [side(2 + e, cols(TE, EDGE * e, EDGE), HE.at[:, :, e]) for e in (near, 1 - near)]
        ring = side(SIDE, (PK.at[0], PK.at[1]), HP)
        everything = mids + edges + [ring]
        v_near, v_far = v_copy(near), v_copy(1 - near)

        def edge(e, pair):
            for h in HALVES:
                TE[h, pl.ds((EDGE + 2) * e, STRIP)] = T[h, pl.ds((M + 1) * e, STRIP)] + V[e, h]
                TE[h, pl.ds(STRIP + 2 * e, 2)] = T[h, pl.ds(STRIP + 2 * EDGE * e, 2)]
            go(pair)

        first = m == 0
        c0, c3 = LAST * near, LAST * (1 - near)
        for h in HALVES:
            G1d[mine_y, h] = pqs[h][None]
        each(d1, "start")
        out = product((LAST * CHUNK + BT) * near, CHUNK + BT)
        put_t(out[BT:], c0)
        for h in HALVES:
            G1a[mine_y, h] = out[0:SUB, lanes(h)][None]
        each(a1, "start")
        pl.when(inner)(v_near.start)
        pl.when(jnp.logical_not(inner))(lambda: edge(near, edges[0]))
        put_t(product(BT + CHUNK, CHUNK), 1)
        go(mids[0])
        half_sum(G1d, G2d, d1, d2)
        put_t(product(BT + 2 * CHUNK, CHUNK), 2)
        go(mids[1])
        each(a1, "wait")
        each(a2, "start")

        pq = full_sum(G2d, d2)
        alpha = [jnp.where(first, -1.0, row(cst[0, h], 0) / row(pq[h], 0)) for h in HALVES]
        tot = [[zero, zero] for h in HALVES]

        def update(c, inside):
            for h in HALVES:
                for k in range(ROWS):
                    i = 1 + ROWS * c + k
                    rn = r[h, i] - alpha[h] * Q[h, i]
                    ln = l[h, i] - alpha[h] * T[h, i]
                    r[h, i] = rn
                    l[h, i] = ln
                    x[h, i] = x[h, i] + alpha[h] * p[h, i]
                    w = colf if inside else jnp.where((i >= OWN) & (i < OWN + M), 1.0, 0.0) * colf
                    tot[h][0] = tot[h][0] + rn * ln
                    tot[h][1] = tot[h][1] + w * (rn * rn)

        out = product(BT + (LAST * CHUNK + BT) * (1 - near), CHUNK)
        update(c0, False)
        update(1, True)
        update(2, True)
        put_t(out, c3)
        v_far.start()
        G2a[mine_x] = G1a[...][None]
        each(a2, "wait_send")
        update(c3, False)
        for h in HALVES:
            G1b[mine_y, h] = jnp.where(sub8 == 0, colsum(tot[h][0]), jnp.where(sub8 == 1, colsum(tot[h][1]), 0.0))[None]
        each(b1, "start")

        @pl.when(inner)
        def _():
            v_near.wait_send()
            rc(T.at[:, pl.ds(1, STRIP)], V.at[near], v_s.at[near], v_r.at[near], left).wait_recv()
            edge(near, edges[0])

        v_far.wait_send()
        rc(T.at[:, pl.ds(1, STRIP)], V.at[1 - near], v_s.at[near], v_r.at[1 - near], left).wait_recv()
        edge(1 - near, edges[1])
        for h in HALVES:
            for i in range(1, ME + 1):
                src, k = (TE, i) if i < EDGE else ((T, i) if i < M - 1 else (TE, i - 2 * ROWS))
                PK[0, h, i - 1:i] = src[h, k, SUB:SUB + 1]
                PK[1, h, i - 1:i] = src[h, k, M - 1:M]
        go(ring)

        each(a2, "wait_recv")
        cq = jnp.concatenate([G2a[:, :, h].reshape(LANES, LANES) for h in HALVES], axis=1)
        yq = dot_pieces(lambda at: Ccat[:, at:at + TILE], cq)
        rzc = []
        for h in HALVES:
            cr[h] = cr[h] - alpha[h] * cq[:, lanes(h)]
            wr[h] = wr[h] - alpha[h] * yq[:, lanes(h)]
            rzc.append(colsum(cr[h] * wr[h]))
        n = LOW // 2
        for part in HALVES:
            o = dot_pieces(lambda at: Ecat[ME * n * part:ME * n * (part + 1), at:at + TILE], yq)
            for h in HALVES:
                Ey[h, n * part:n * (part + 1)] = o[:, lanes(h)].reshape(n, ME, LANES)

        half_sum(G1b, G2b, b1, b2)
        got = full_sum(G2b, b2)
        beta = []
        for h in HALVES:
            rzn = row(got[h], 0) + rzc[h]
            rr = row(got[h], 1)
            beta.append(jnp.where(first, 0.0, rzn / row(cst[0, h], 0)))
            ff = jnp.where(first, jnp.sqrt(rr), row(cst[1, h], 0))
            cst[0, h] = wide(rzn)
            cst[1, h] = wide(ff)
            nrm_ref[:, lanes(h)] = jnp.where(sub8 == m - 1, jnp.sqrt(rr) / ff, nrm_ref[:, lanes(h)])

        for pair in everything:
            pl.when(has_right)(pair[0].wait_recv)
            pl.when(has_left)(pair[1].wait_recv)

        def renew(i, u):
            for h in HALVES:
                zn = z[h, i] - alpha[h] * (u[h] + Ey[h, i])
                z[h, i] = zn
                p[h, i] = zn + beta[h] * p[h, i]

        def sides(b, buf, n, h, k):
            return jnp.concatenate([b[0:SUB] + buf[par, 0, n, h, k], b[SUB:M], b[M:] + buf[par, 1, n, h, k]], axis=0)

        def mid_rows(k, c):
            for n in HALVES:
                i = EDGE + ROWS * n + k
                renew(i, [sides(T[h, i], HB, n, h, k) for h in HALVES])
            return c
        lax.fori_loop(0, ROWS, mid_rows, 0)

        def edge_rows(k, c):
            for n in HALVES:
                renew((M - 1) * n + k, [sides(TE[h, EDGE * n + k], HE, n, h, k) for h in HALVES])
            return c
        lax.fori_loop(0, EDGE, edge_rows, 0)
        for j in HALVES:
            renew(LOW - 2 + j, [HP[par, j, h] for h in HALVES])

        def apply_rows(g, car):
            sums = list(car)
            for h in HALVES:
                lring, rring = [p[h, LOW - 2 + j, pl.ds(mult(SUB * g, SUB), SUB), :] for j in HALVES]
                rows = []
                for k in range(SUB):
                    i = SUB * g + k
                    c = p[h, i + 1]
                    west = jnp.where(jcol == 0, row(lring, k), pltpu.roll(c, 1, 0))
                    east = jnp.where(jcol == ME - 1, row(rring, k), pltpu.roll(c, ME - 1, 0))
                    q = W5[SIDE, i] * c
                    for j, other in enumerate((p[h, i], p[h, i + 2], west, east)):
                        q = q - W5[j, i] * other
                    Q[h, i + 1] = q
                    sums[h] = sums[h] + jnp.where((i >= D) & (i < D + M), 1.0, 0.0) * colf * (c * q)
                    rows.append(q)
                    if len(rows) == 2:
                        put_x(rows, h, D * g + k // 2)
                        rows = []
            return tuple(sums)
        car = lax.fori_loop(0, ME // SUB - 1, apply_rows, (zero, zero))
        car = apply_rows(ME // SUB - 1, car)
        for h in HALVES:
            pqs[h] = wide(colsum(car[h]))

        for pair in everything:
            pl.when(has_left)(pair[0].wait_send)
            pl.when(has_right)(pair[1].wait_send)
        return carry

    lax.fori_loop(0, ITERS, step, 0)

    for h in HALVES:
        G1d[mine_y, h] = pqs[h][None]
    each(d1, "start")
    half_sum(G1d, G2d, d1, d2)
    pq = full_sum(G2d, d2)
    alpha = [row(cst[0, h], 0) / row(pq[h], 0) for h in HALVES]

    def finish(i, car):
        res = []
        for h in HALVES:
            rn = r[h, i] - alpha[h] * Q[h, i]
            res.append(car[h] + colf * (rn * rn))
            xn = x[h, i] + alpha[h] * p[h, i]
            T[h, i, 0:M] = pltpu.roll(jnp.concatenate([xn, xn[0:SUB]], axis=0), WIDE - D, 0)[0:M]
        return tuple(res)
    rr = lax.fori_loop(OWN, OWN + M, finish, (zero, zero))
    out_cp = [pltpu.make_async_copy(T.at[h, own, pl.ds(0, M)], x_hbm.at[:, :, pl.ds(LANES * h, LANES)], out_sem.at[h]) for h in HALVES]
    each(out_cp, "start")
    for h in HALVES:
        G1b[mine_y, h] = wide(colsum(rr[h]))[None]
    each(b1, "start")
    half_sum(G1b, G2b, b1, b2)
    got = full_sum(G2b, b2)
    for h in HALVES:
        nrm_ref[:, lanes(h)] = jnp.where(sub8 == ITERS - 1, jnp.sqrt(row(got[h], 0)) / row(cst[1, h], 0), nrm_ref[:, lanes(h)])
    each(out_cp, "wait")


def solution(mesh):
    def dma(*shape):
        return pltpu.SemaphoreType.DMA(shape)

    def vm(*shape, dtype=F32):
        return pltpu.VMEM(shape, dtype)

    field = vm(2, LOW, ME, LANES)
    strips = [vm(2, 2, 2, 2, n, SUB, LANES) for n in (ROWS, EDGE)]
    gathers = [vm(SIDE, 2, SUB, LANES), vm(SIDE, SIDE, 2, SUB, LANES)] + [vm(SIDE, 2, SUB, LANES)] * SIDE
    scratch = [
        vm(SIDE, M + 2 * OWN, WIDE, LANES), vm(NL, KM * len(PIECES), dtype=BF16), vm(NL, 2 * TILE, dtype=BF16),
        vm(SIDE, CHUNK, NE), vm(len(PIECES), KM, TILE, dtype=BF16), vm(2 * TILE, TILE, dtype=BF16),
        field, vm(2, 2 * EDGE, ME, LANES), field, field, field, field, field, field, field,
        vm(SIDE + 1, ME, ME, LANES), vm(LOW * ME, LANES * len(PIECES), dtype=BF16), vm(2, ME, LANES),
        vm(2, 2, STRIP, ME, LANES), *strips, vm(2, 2, 2, ME, LANES), vm(2, 2, ME, LANES), *gathers,
        vm(LANES, LANES * len(PIECES), dtype=BF16), vm(2, LANES, LANES), vm(2, LANES, LANES), vm(2, 2, SUB, LANES),
        vm(2, SUB, LANES), dma(SIDE), dma(SIDE), *[dma(2)] * 6, *[dma(2, 2, SIDE + 1)] * 2, *[dma(LAST)] * 12, dma(2),
    ]
    any_spec = pl.BlockSpec(memory_space=pl.ANY)
    vmem_spec = pl.BlockSpec(memory_space=pltpu.VMEM)

    def body(forcing, kappa, local_inv, coarse_basis, coarse_counts, coarse_inv):
        index = lax.axis_index("sx") * SIDE + lax.axis_index("sy")
        basis = coarse_basis[0]
        mine = jnp.arange(LANES) // KMAX == index
        spread = jnp.where(mine[None, :], jnp.tile(basis, (1, LANES // KMAX)), 0.0)
        aux = jnp.stack([spread.reshape(M, M, LANES), jnp.broadcast_to(kappa[:, :, None], (M, M, LANES))])
        bt = jnp.pad(basis.T.reshape(KMAX, M, M), ((0, BT - KMAX), (D, D), (D, D))).reshape(BT, NE)
        cnt = jnp.broadcast_to(jnp.where(mine, coarse_counts.astype(F32), 0.0)[None, :], (SUB, LANES))
        return pl.pallas_call(
            solve_kernel,
            out_shape=(jax.ShapeDtypeStruct((M, M, 2 * LANES), F32), jax.ShapeDtypeStruct((ITERS, 2 * LANES), F32)),
            in_specs=[any_spec] * len(PIECES) + [vmem_spec] * len(PIECES),
            out_specs=(any_spec, vmem_spec),
            scratch_shapes=scratch,
            compiler_params=pltpu.CompilerParams(collective_id=0, has_side_effects=True, vmem_limit_bytes=67043328),
        )(forcing, aux, local_inv[0], bt, coarse_inv, cnt)

    cell_spec = P(("batch", "sx"), "sy", None)
    sub_spec = P(("batch", "sx", "sy"), None, None)
    return jax.shard_map(body, mesh=mesh, in_specs=(cell_spec, P(("batch", "sx"), "sy"), sub_spec, sub_spec, P(("batch", "sx", "sy")), P("batch", None)), out_specs=(cell_spec, P("batch", None)), check_vma=False)
```

```python
import jax
import jax.numpy as jnp
from jax import lax
from jax.experimental import pallas as pl
from jax.experimental.pallas import tpu as pltpu
from jax.sharding import PartitionSpec as P

ITERS = 8
M = 32
D = 4
ME = M + 2 * D
NE = ME * ME
SUB = 8
LANES = 128
TILE = 256
KT = NE // TILE
KM = KT * TILE
REM = NE - KM
ROWS = 10
CHUNK = ROWS * ME
NA = 208
BT = 16
NL = NE + 2 * BT
KMAX = 8
GRID = 128
LOW = M + SUB + D
WIDE = M + 2 * SUB
OWN = D + 1
STRIP = 9
EDGE = STRIP + 2
MESH = pl.DeviceIdType.MESH
HI = lax.Precision.HIGHEST
F32 = jnp.float32
BF16 = jnp.bfloat16
HALVES = (0, 1)
PIECES = (0, 1, 2)
FAR = (1, 2, 3)
LAST = FAR[-1]
SIDE = FAR[-1] + 1


def lanes(h):
    return slice(LANES * h, LANES * (h + 1))


def tile(k):
    return slice(TILE * k, TILE * (k + 1))


def mult(v, n=BT):
    return v if isinstance(v, int) else pl.multiple_of(v, n)


def row(v, k):
    return v[k:k + 1]


def wide(v):
    return jnp.broadcast_to(v, (SUB, LANES))


def colsum(v):
    return jnp.sum(v, axis=0, keepdims=True)


def each(copies, what):
    for c in copies:
        getattr(c, what)()


def split3(v):
    hi = v.astype(BF16)
    rest = v - hi.astype(F32)
    mid = rest.astype(BF16)
    low = (rest - mid.astype(F32)).astype(BF16)
    return hi, mid, low


def solve_kernel(f_hbm, aux_hbm, inv_hbm, bt_ref, cinv_ref, cnt_ref, x_hbm, nrm_ref,
                 S48, L, Lr, stage, X, Xr, T, TE, z, p, r, l, x, Q, Ey, W5, Ecat, RE,
               V, HB, HE, HP, PK, G1a, G2a, G1b, G2b, G1d, G2d, Ccat, cr, wr, cst, pqs,
               ld_sem, own_sem, h0_s, h0_r, v0_s, v0_r, v_s, v_r, hm_s, hm_r,
               a1_s, a1_r, a2_s, a2_r, b1_s, b1_r, b2_s, b2_r, d1_s, d1_r, d2_s, d2_r, out_sem):
    sx = lax.axis_index("sx")
    sy = lax.axis_index("sy")
    left, right = {"sy": sy - 1}, {"sy": sy + 1}
    has_left, has_right = sy > 0, sy < LAST
    has = (sx > 0, sx < LAST)
    near = lax.rem(sx, 2)
    inner = (sx > 0) & (sx < LAST)

    def rc(src, dst, s, q, dev):
        return pltpu.make_async_remote_copy(src, dst, s, q, device_id=dev, device_id_type=MESH)

    own = pl.ds(OWN, M)
    inv_cp = [pltpu.make_async_copy(inv_hbm.at[pl.ds(CHUNK * c, CHUNK)], stage.at[c], ld_sem.at[c]) for c in range(SIDE)]
    own_cp = [pltpu.make_async_copy(f_hbm.at[:, :, pl.ds(LANES * h, LANES)], S48.at[h, own, pl.ds(SUB, M)], own_sem.at[h]) for h in HALVES]
    own_cp += [pltpu.make_async_copy(aux_hbm.at[h], S48.at[2 + h, own, pl.ds(SUB, M)], own_sem.at[2 + h]) for h in HALVES]
    each(own_cp, "start")
    each(inv_cp, "start")
    zrow = jnp.zeros((SIDE, OWN, WIDE, LANES), F32)
    S48[:, 0:OWN] = zrow
    S48[:, OWN + M:] = zrow
    zcol = jnp.zeros((SIDE, M, SUB, LANES), F32)
    S48[:, OWN:OWN + M, 0:SUB] = zcol
    S48[:, OWN:OWN + M, ME:] = zcol
    for b in (V, HB, HE, HP):
        b[...] = jnp.zeros(b.shape, F32)

    bar = pltpu.get_barrier_semaphore()
    for d in FAR:
        pl.semaphore_signal(bar, inc=1, device_id={"sx": lax.rem(sx + d, SIDE)}, device_id_type=MESH)
        pl.semaphore_signal(bar, inc=1, device_id={"sy": lax.rem(sy + d, SIDE)}, device_id_type=MESH)
    pl.semaphore_wait(bar, 2 * LAST)

    def first_copies(G1, s, q):
        return [rc(G1.at[sy], G1.at[sy], s.at[d - 1], q.at[d - 1], {"sy": lax.rem(sy + d, SIDE)}) for d in FAR]

    def second_copies(src, G2, s, q):
        return [rc(src, G2.at[sx], s.at[d - 1], q.at[d - 1], {"sx": lax.rem(sx + d, SIDE)}) for d in FAR]

    a1 = first_copies(G1a, a1_s, a1_r)
    a2 = second_copies(G1a, G2a, a2_s, a2_r)
    b1 = first_copies(G1b, b1_s, b1_r)
    b2 = second_copies(G2b.at[sx], G2b, b2_s, b2_r)
    d1 = first_copies(G1d, d1_s, d1_r)
    d2 = second_copies(G2d.at[sx], G2d, d2_s, d2_r)
    mine_y, mine_x = pl.ds(sy, 1), pl.ds(sx, 1)

    def half_sum(G1, G2, one, two):
        each(one, "wait")
        G2[mine_x] = jnp.sum(G1[...], axis=0, keepdims=True)
        each(two, "start")

    def full_sum(G2, two):
        each(two, "wait")
        return jnp.sum(G2[...], axis=0)

    G1b[mine_y] = jnp.broadcast_to(cnt_ref[...], (1, 2, SUB, LANES))
    each(b1, "start")

    each(own_cp, "wait")
    h0l = rc(S48.at[:, own, pl.ds(SUB, SUB)], S48.at[:, own, pl.ds(ME, SUB)], h0_s.at[0], h0_r.at[0], left)
    h0r = rc(S48.at[:, own, pl.ds(M, SUB)], S48.at[:, own, pl.ds(0, SUB)], h0_s.at[1], h0_r.at[1], right)
    v0 = [rc(S48.at[:, pl.ds(OWN, OWN)], S48.at[:, pl.ds(OWN + M, OWN)], v0_s.at[0], v0_r.at[1], {"sx": sx - 1}),
          rc(S48.at[:, pl.ds(M, OWN)], S48.at[:, pl.ds(0, OWN)], v0_s.at[1], v0_r.at[0], {"sx": sx + 1})]
    v0_in = [rc(S48.at[:, pl.ds(0, OWN)], S48.at[:, pl.ds(0, OWN)], v0_s.at[e], v0_r.at[e], left) for e in HALVES]
    pl.when(has_left)(h0l.start)
    pl.when(has_right)(h0r.start)

    for b in (p, z, r, l, x, T):
        def zero(i, c, b=b):
            b[:, pl.ds(i, 1)] = jnp.zeros((2, 1, ME, LANES), F32)
            return c
        lax.fori_loop(0, b.shape[1], zero, 0)
    Xr[...] = jnp.zeros(Xr.shape, BF16)
    for b in (cr, wr, cst, pqs, nrm_ref):
        b[...] = jnp.zeros(b.shape, F32)

    def put_l(v, rows):
        one, two, three = split3(v)
        rest = []
        for k, piece in enumerate((one, two, three)):
            L[rows, KM * k:KM * (k + 1)] = piece[:, 0:KM]
            rest.append(piece[:, KM:].astype(F32))
        twice = jnp.concatenate(rest[0:2], axis=1).astype(BF16)
        Lr[rows, lanes(0)] = twice
        Lr[rows, lanes(1)] = twice
        Lr[rows, lanes(2)] = jnp.concatenate([rest[0], rest[2]], axis=1).astype(BF16)
        Lr[rows, lanes(LAST)] = jnp.zeros(twice.shape, BF16)

    for at in (0, LAST * CHUNK + BT):
        put_l(bt_ref[...], pl.ds(at, BT))
    half_sum(G1b, G2b, b1, b2)

    def split_inv(c):
        inv_cp[c].wait()

        def body(k, carry):
            put_l(stage[c, pl.ds(mult(BT * k), BT), :], pl.ds(mult(CHUNK * c + BT * (c // LAST + 1) + BT * k), BT))
            return carry
        lax.fori_loop(0, CHUNK // BT, body, 0)

    split_inv(0)
    split_inv(1)
    pl.when(has_left)(h0l.wait_send)
    pl.when(has_right)(h0r.wait_send)
    pl.when(has_right)(h0l.wait_recv)
    pl.when(has_left)(h0r.wait_recv)
    for e in HALVES:
        pl.when(has[e])(v0[e].start)
    split_inv(2)
    split_inv(LAST)

    def dot(a, b):
        return jnp.dot(a, b, preferred_element_type=F32)

    def dot_pieces(lhs, v):
        y1, y2, y3 = split3(v)
        total = 0.0
        for n, two in enumerate(((y1, y1), (y2, y2), (y3, y1))):
            total = total + dot(lhs(LANES * (n // 2)), jnp.concatenate(two, axis=0))
        return total

    cnt = full_sum(G2b, b2)[0]
    lane = lax.broadcasted_iota(jnp.int32, (SUB, LANES), 1)
    starts = cnt
    for d in (KMAX, 2 * KMAX, D * KMAX, SUB * KMAX):
        starts = starts + jnp.where(lane >= d, pltpu.roll(starts, d, 1), 0.0)
    starts = starts - cnt
    col = (lane % KMAX).astype(F32)
    target = jnp.where(col < cnt, starts + col, -1.0)
    half = cinv_ref.shape[0]
    pick = jnp.where(lax.broadcasted_iota(jnp.int32, (half, LANES), 0).astype(F32) == row(target, 0), 1.0, 0.0)

    def rhs_of(parts):
        v = jnp.concatenate(parts + [jnp.zeros_like(parts[0])], axis=0)
        return v.astype(BF16)

    def lhs_of(parts):
        v = jnp.concatenate(parts + [jnp.zeros_like(parts[0])], axis=1)
        return v.astype(BF16)

    def as_f32(v):
        return [piece.astype(F32) for piece in split3(v)]
    spread = dot(lhs_of(as_f32(cinv_ref[...])), rhs_of([pick] * len(PIECES)))
    spread = dot(lhs_of([pick.T] * len(PIECES)), rhs_of(as_f32(spread)))

    def put_middle(ref, rows, v):
        for k, piece in zip((1, 0, 2), split3(v)):
            ref[rows, lanes(k)] = piece
    put_middle(Ccat, pl.ds(0, LANES), spread)

    for e in HALVES:
        pl.when(has[e])(v0[e].wait_send)
        pl.when(has[e])(v0_in[e].wait_recv)

    jcol = lax.broadcasted_iota(jnp.int32, (ME, LANES), 0)
    gj = sy * M + jcol - D
    in_col = (gj >= 0) & (gj < GRID)

    def shifted(v, k=D):
        return pltpu.roll(v, WIDE - k, 0)[0:ME]

    def weights(i, c):
        gi = sx * M + i - D
        ok = in_col & (gi >= 0) & (gi < GRID)
        here = S48[LAST, i + 1]
        kc = shifted(here)

        def pair(other, inside):
            both = ok & inside
            w = jnp.where(both, 2.0 * kc * other / jnp.where(both, kc + other, 1.0), 0.0)
            return w, jnp.where(ok & jnp.logical_not(inside), kc, w)
        edges = (pair(shifted(S48[LAST, i]), ok & (gi > 0)), pair(shifted(S48[LAST, i + 2]), ok & (gi < GRID - 1)),
                 pair(shifted(here, D - 1), gj > 0), pair(shifted(here, D + 1), gj < GRID - 1))
        total = 0.0
        for k, (w, d) in enumerate(edges):
            W5[k, i] = w
            total = total + d
        W5[SIDE, i] = total
        return c
    lax.fori_loop(0, ME, weights, 0)

    for i in range(ME):
        RE[0, i:i + 1] = S48[2, i + 1, D - 1:D]
        RE[1, i:i + 1] = S48[2, i + 1, LOW:LOW + 1]

    def pair_of(two, k):
        return jnp.concatenate(two, axis=0), pl.ds(mult(2 * ME * k), 2 * ME)

    def basis_rows(k, c):
        v, rows = pair_of([shifted(S48[2, 2 * k]), shifted(S48[2, 2 * k + 1])], k)
        put_middle(Ecat, rows, v)
        return c
    lax.fori_loop(0, LOW // 2 - 1, basis_rows, 0)
    v, rows = pair_of([RE[0], RE[1]], LOW // 2 - 1)
    put_middle(Ecat, rows, v)

    def put_x(two, h, k):
        v, rows = pair_of(two, k)
        pieces = split3(v)
        if isinstance(k, int) and k == ME // 2 - 1:
            n = KM - 2 * ME * k
            for j, piece in enumerate(pieces):
                X[j, KM - n:KM, lanes(h)] = piece[0:n]
            for slot, j in enumerate((0, 0, 1, 1, 2, 0)):
                Xr[REM * slot:REM * (slot + 1), lanes(h)] = pieces[j][n:]
        else:
            for j, piece in enumerate(pieces):
                X[j, rows, lanes(h)] = piece

    def first_rows(k, c):
        for h in HALVES:
            two = [shifted(S48[h, 2 * k + 1 + j]) for j in HALVES]
            for j in HALVES:
                Q[h, 2 * k + 1 + j] = two[j]
            put_x(two, h, k)
        return c
    lax.fori_loop(0, ME // 2 - 1, first_rows, 0)
    first_rows(ME // 2 - 1, 0)

    colf = jnp.where((jcol >= D) & (jcol < D + M), 1.0, 0.0)
    sub8 = lax.broadcasted_iota(jnp.int32, (SUB, LANES), 0)
    zero = jnp.zeros((ME, LANES), F32)

    def product(start, n):
        first = NA
        outs = []
        for at, size in ((0, first), (first, n - first)):
            rows = pl.ds(mult(start + at), size)
            total = dot(Lr[rows, :], Xr[...])
            for j in PIECES:
                for i in PIECES[:len(PIECES) - j]:
                    total = total + dot(L[rows, KM * i:KM * (i + 1)], X[j])
            outs.append(total)
        return outs

    def put_t(outs, c):
        at = 0
        for v in outs:
            while v.shape[0]:
                top, off = 1 + ROWS * c + at // ME, at % ME
                n = min(ME - off, v.shape[0]) if off or v.shape[0] < ME else v.shape[0] // ME * ME
                whole = max(n // ME, 1)
                for h in HALVES:
                    T[h, pl.ds(top, whole), off:off + n // whole] = v[0:n, lanes(h)].reshape(whole, n // whole, LANES)
                v, at = v[n:], at + n

    def v_copy(e):
        return rc(T.at[:, pl.ds(1 + (M - 1) * e, STRIP)], V.at[1 - e], v_s.at[e], v_r.at[1 - e], {"sx": sx - 1 + 2 * e})

    def step(m, carry):
        par = lax.rem(m, 2)

        def side(n, src, dst):
            return [rc(src[j], dst.at[par, 1 - j], hm_s.at[par, j, n], hm_r.at[par, 1 - j, n], (left, right)[j]) for j in HALVES]

        def go(pair):
            pl.when(has_left)(pair[0].start)
            pl.when(has_right)(pair[1].start)

        def cols(ref, lo, n):
            return [ref.at[:, pl.ds(lo, n), pl.ds(M * j, SUB)] for j in HALVES]

        mids = [side(n, cols(T, EDGE + ROWS * n, ROWS), HB.at[:, :, n]) for n in HALVES]
        edges = [side(2 + e, cols(TE, EDGE * e, EDGE), HE.at[:, :, e]) for e in (near, 1 - near)]
        ring = side(SIDE, (PK.at[0], PK.at[1]), HP)
        everything = mids + edges + [ring]
        v_near, v_far = v_copy(near), v_copy(1 - near)

        def edge(e, pair):
            for h in HALVES:
                TE[h, pl.ds((EDGE + 2) * e, STRIP)] = T[h, pl.ds((M + 1) * e, STRIP)] + V[e, h]
                TE[h, pl.ds(STRIP + 2 * e, 2)] = T[h, pl.ds(STRIP + 2 * EDGE * e, 2)]
            go(pair)

        first = m == 0
        c0, c3 = LAST * near, LAST * (1 - near)
        for h in HALVES:
            G1d[mine_y, h] = pqs[h][None]
        each(d1, "start")
        out = product((LAST * CHUNK + BT) * near, CHUNK + BT)
        put_t([out[0][BT:], out[1]], c0)
        for h in HALVES:
            G1a[mine_y, h] = out[0][0:SUB, lanes(h)][None]
        each(a1, "start")
        pl.when(inner)(v_near.start)
        pl.when(jnp.logical_not(inner))(lambda: edge(near, edges[0]))
        put_t(product(BT + CHUNK, CHUNK), 1)
        go(mids[0])
        half_sum(G1d, G2d, d1, d2)
        put_t(product(BT + 2 * CHUNK, CHUNK), 2)
        go(mids[1])
        each(a1, "wait")
        each(a2, "start")

        pq = full_sum(G2d, d2)
        alpha = [jnp.where(first, -1.0, row(cst[0, h], 0) / row(pq[h], 0)) for h in HALVES]
        tot = [[zero, zero] for h in HALVES]

        def update(c, inside):
            for h in HALVES:
                for k in range(ROWS):
                    i = 1 + ROWS * c + k
                    rn = r[h, i] - alpha[h] * Q[h, i]
                    ln = l[h, i] - alpha[h] * T[h, i]
                    r[h, i] = rn
                    l[h, i] = ln
                    x[h, i] = x[h, i] + alpha[h] * p[h, i]
                    w = colf if inside else jnp.where((i >= OWN) & (i < OWN + M), 1.0, 0.0) * colf
                    tot[h][0] = tot[h][0] + rn * ln
                    tot[h][1] = tot[h][1] + w * (rn * rn)

        out = product(BT + (LAST * CHUNK + BT) * (1 - near), CHUNK)
        update(c0, False)
        update(1, True)
        update(2, True)
        put_t(out, c3)
        v_far.start()
        G2a[mine_x] = G1a[...][None]
        each(a2, "wait_send")
        update(c3, False)
        for h in HALVES:
            G1b[mine_y, h] = jnp.where(sub8 == 0, colsum(tot[h][0]), jnp.where(sub8 == 1, colsum(tot[h][1]), 0.0))[None]
        each(b1, "start")

        @pl.when(inner)
        def _():
            v_near.wait_send()
            rc(T.at[:, pl.ds(1, STRIP)], V.at[near], v_s.at[near], v_r.at[near], left).wait_recv()
            edge(near, edges[0])

        v_far.wait_send()
        rc(T.at[:, pl.ds(1, STRIP)], V.at[1 - near], v_s.at[near], v_r.at[1 - near], left).wait_recv()
        edge(1 - near, edges[1])
        for h in HALVES:
            for i in range(1, ME + 1):
                src, k = (TE, i) if i < EDGE else ((T, i) if i < M - 1 else (TE, i - 2 * ROWS))
                PK[0, h, i - 1:i] = src[h, k, SUB:SUB + 1]
                PK[1, h, i - 1:i] = src[h, k, M - 1:M]
        go(ring)

        each(a2, "wait_recv")
        cq = jnp.concatenate([G2a[:, :, h].reshape(LANES, LANES) for h in HALVES], axis=1)
        yq = dot_pieces(lambda at: Ccat[:, at:at + TILE], cq)
        rzc = []
        for h in HALVES:
            cr[h] = cr[h] - alpha[h] * cq[:, lanes(h)]
            wr[h] = wr[h] - alpha[h] * yq[:, lanes(h)]
            rzc.append(colsum(cr[h] * wr[h]))
        n = LOW // 2
        for part in HALVES:
            o = dot_pieces(lambda at: Ecat[ME * n * part:ME * n * (part + 1), at:at + TILE], yq)
            for h in HALVES:
                Ey[h, n * part:n * (part + 1)] = o[:, lanes(h)].reshape(n, ME, LANES)

        half_sum(G1b, G2b, b1, b2)
        got = full_sum(G2b, b2)
        beta = []
        for h in HALVES:
            rzn = row(got[h], 0) + rzc[h]
            rr = row(got[h], 1)
            beta.append(jnp.where(first, 0.0, rzn / row(cst[0, h], 0)))
            ff = jnp.where(first, jnp.sqrt(rr), row(cst[1, h], 0))
            cst[0, h] = wide(rzn)
            cst[1, h] = wide(ff)
            nrm_ref[:, lanes(h)] = jnp.where(sub8 == m - 1, jnp.sqrt(rr) / ff, nrm_ref[:, lanes(h)])

        for pair in everything:
            pl.when(has_right)(pair[0].wait_recv)
            pl.when(has_left)(pair[1].wait_recv)

        def renew(i, u):
            for h in HALVES:
                zn = z[h, i] - alpha[h] * (u[h] + Ey[h, i])
                z[h, i] = zn
                p[h, i] = zn + beta[h] * p[h, i]

        def sides(b, buf, n, h, k):
            return jnp.concatenate([b[0:SUB] + buf[par, 0, n, h, k], b[SUB:M], b[M:] + buf[par, 1, n, h, k]], axis=0)

        def mid_rows(k, c):
            for n in HALVES:
                i = EDGE + ROWS * n + k
                renew(i, [sides(T[h, i], HB, n, h, k) for h in HALVES])
            return c
        lax.fori_loop(0, ROWS, mid_rows, 0)

        def edge_rows(k, c):
            for n in HALVES:
                renew((M - 1) * n + k, [sides(TE[h, EDGE * n + k], HE, n, h, k) for h in HALVES])
            return c
        lax.fori_loop(0, EDGE, edge_rows, 0)
        for j in HALVES:
            renew(LOW - 2 + j, [HP[par, j, h] for h in HALVES])

        def apply_rows(g, car):
            sums = list(car)
            for h in HALVES:
                lring, rring = [p[h, LOW - 2 + j, pl.ds(mult(SUB * g, SUB), SUB), :] for j in HALVES]
                rows = []
                for k in range(SUB):
                    i = SUB * g + k
                    c = p[h, i + 1]
                    west = jnp.where(jcol == 0, row(lring, k), pltpu.roll(c, 1, 0))
                    east = jnp.where(jcol == ME - 1, row(rring, k), pltpu.roll(c, ME - 1, 0))
                    q = W5[SIDE, i] * c
                    for j, other in enumerate((p[h, i], p[h, i + 2], west, east)):
                        q = q - W5[j, i] * other
                    Q[h, i + 1] = q
                    sums[h] = sums[h] + jnp.where((i >= D) & (i < D + M), 1.0, 0.0) * colf * (c * q)
                    rows.append(q)
                    if len(rows) == 2:
                        put_x(rows, h, D * g + k // 2)
                        rows = []
            return tuple(sums)
        car = lax.fori_loop(0, ME // SUB - 1, apply_rows, (zero, zero))
        car = apply_rows(ME // SUB - 1, car)
        for h in HALVES:
            pqs[h] = wide(colsum(car[h]))

        for pair in everything:
            pl.when(has_left)(pair[0].wait_send)
            pl.when(has_right)(pair[1].wait_send)
        return carry

    lax.fori_loop(0, ITERS, step, 0)

    for h in HALVES:
        G1d[mine_y, h] = pqs[h][None]
    each(d1, "start")
    half_sum(G1d, G2d, d1, d2)
    pq = full_sum(G2d, d2)
    alpha = [row(cst[0, h], 0) / row(pq[h], 0) for h in HALVES]

    def finish(i, car):
        res = []
        for h in HALVES:
            rn = r[h, i] - alpha[h] * Q[h, i]
            res.append(car[h] + colf * (rn * rn))
            xn = x[h, i] + alpha[h] * p[h, i]
            T[h, i, 0:M] = pltpu.roll(jnp.concatenate([xn, xn[0:SUB]], axis=0), WIDE - D, 0)[0:M]
        return tuple(res)
    rr = lax.fori_loop(OWN, OWN + M, finish, (zero, zero))
    out_cp = [pltpu.make_async_copy(T.at[h, own, pl.ds(0, M)], x_hbm.at[:, :, pl.ds(LANES * h, LANES)], out_sem.at[h]) for h in HALVES]
    each(out_cp, "start")
    for h in HALVES:
        G1b[mine_y, h] = wide(colsum(rr[h]))[None]
    each(b1, "start")
    half_sum(G1b, G2b, b1, b2)
    got = full_sum(G2b, b2)
    for h in HALVES:
        nrm_ref[:, lanes(h)] = jnp.where(sub8 == ITERS - 1, jnp.sqrt(row(got[h], 0)) / row(cst[1, h], 0), nrm_ref[:, lanes(h)])
    each(out_cp, "wait")


def solution(mesh):
    def dma(*shape):
        return pltpu.SemaphoreType.DMA(shape)

    def vm(*shape, dtype=F32):
        return pltpu.VMEM(shape, dtype)

    field = vm(2, LOW, ME, LANES)
    strips = [vm(2, 2, 2, 2, n, SUB, LANES) for n in (ROWS, EDGE)]
    gathers = [vm(SIDE, 2, SUB, LANES), vm(SIDE, SIDE, 2, SUB, LANES)] + [vm(SIDE, 2, SUB, LANES)] * SIDE
    scratch = [
        vm(SIDE, M + 2 * OWN, WIDE, LANES), vm(NL, KM * len(PIECES), dtype=BF16), vm(NL, 2 * TILE, dtype=BF16),
        vm(SIDE, CHUNK, NE), vm(len(PIECES), KM, TILE, dtype=BF16), vm(2 * TILE, TILE, dtype=BF16),
        field, vm(2, 2 * EDGE, ME, LANES), field, field, field, field, field, field, field,
        vm(SIDE + 1, ME, ME, LANES), vm(LOW * ME, LANES * len(PIECES), dtype=BF16), vm(2, ME, LANES),
        vm(2, 2, STRIP, ME, LANES), *strips, vm(2, 2, 2, ME, LANES), vm(2, 2, ME, LANES), *gathers,
        vm(LANES, LANES * len(PIECES), dtype=BF16), vm(2, LANES, LANES), vm(2, LANES, LANES), vm(2, 2, SUB, LANES),
        vm(2, SUB, LANES), dma(SIDE), dma(SIDE), *[dma(2)] * 6, *[dma(2, 2, SIDE + 1)] * 2, *[dma(LAST)] * 12, dma(2),
    ]
    any_spec = pl.BlockSpec(memory_space=pl.ANY)
    vmem_spec = pl.BlockSpec(memory_space=pltpu.VMEM)

    def body(forcing, kappa, local_inv, coarse_basis, coarse_counts, coarse_inv):
        index = lax.axis_index("sx") * SIDE + lax.axis_index("sy")
        basis = coarse_basis[0]
        mine = jnp.arange(LANES) // KMAX == index
        spread = jnp.where(mine[None, :], jnp.tile(basis, (1, LANES // KMAX)), 0.0)
        aux = jnp.stack([spread.reshape(M, M, LANES), jnp.broadcast_to(kappa[:, :, None], (M, M, LANES))])
        bt = jnp.pad(basis.T.reshape(KMAX, M, M), ((0, BT - KMAX), (D, D), (D, D))).reshape(BT, NE)
        cnt = jnp.broadcast_to(jnp.where(mine, coarse_counts.astype(F32), 0.0)[None, :], (SUB, LANES))
        return pl.pallas_call(
            solve_kernel,
            out_shape=(jax.ShapeDtypeStruct((M, M, 2 * LANES), F32), jax.ShapeDtypeStruct((ITERS, 2 * LANES), F32)),
            in_specs=[any_spec] * len(PIECES) + [vmem_spec] * len(PIECES),
            out_specs=(any_spec, vmem_spec),
            scratch_shapes=scratch,
            compiler_params=pltpu.CompilerParams(collective_id=0, has_side_effects=True, vmem_limit_bytes=67043328),
        )(forcing, aux, local_inv[0], bt, coarse_inv, cnt)

    cell_spec = P(("batch", "sx"), "sy", None)
    sub_spec = P(("batch", "sx", "sy"), None, None)
    return jax.shard_map(body, mesh=mesh, in_specs=(cell_spec, P(("batch", "sx"), "sy"), sub_spec, sub_spec, P(("batch", "sx", "sy")), P("batch", None)), out_specs=(cell_spec, P("batch", None)), check_vma=False)
```

```python
import jax
import jax.numpy as jnp
from jax import lax
from jax.experimental import pallas as pl
from jax.experimental.pallas import tpu as pltpu
from jax.sharding import PartitionSpec as P

ITERS = 8
M = 32
D = 4
ME = M + 2 * D
NE = ME * ME
SUB = 8
LANES = 128
TILE = 256
KT = NE // TILE
KM = KT * TILE
REM = NE - KM
ROWS = 10
CHUNK = ROWS * ME
NP = NE + REM
NA = 208
BT = 16
NL = NE + 2 * BT
KMAX = 8
GRID = 128
LOW = M + SUB + D
WIDE = M + 2 * SUB
OWN = D + 1
STRIP = 9
EDGE = STRIP + 2
MESH = pl.DeviceIdType.MESH
HI = lax.Precision.HIGHEST
F32 = jnp.float32
BF16 = jnp.bfloat16
HALVES = (0, 1)
PIECES = (0, 1, 2)
FAR = (1, 2, 3)
LAST = FAR[-1]
SIDE = FAR[-1] + 1


def lanes(h):
    return slice(LANES * h, LANES * (h + 1))


def tile(k):
    return slice(TILE * k, TILE * (k + 1))


def mult(v, n=BT):
    return v if isinstance(v, int) else pl.multiple_of(v, n)


def row(v, k):
    return v[k:k + 1]


def wide(v):
    return jnp.broadcast_to(v, (SUB, LANES))


def colsum(v):
    return jnp.sum(v, axis=0, keepdims=True)


def each(copies, what):
    for c in copies:
        getattr(c, what)()


def split3(v):
    hi = v.astype(BF16)
    rest = v - hi.astype(F32)
    mid = rest.astype(BF16)
    low = (rest - mid.astype(F32)).astype(BF16)
    return hi, mid, low


def solve_kernel(f_hbm, inv_hbm, own_ref, cinv_ref, cnt_ref, x_hbm, nrm_ref,
                 S48, L, Lr, stage, X, Xr, T, TE, z, p, r, l, x, Q, Ey, W5, Ecat, RE, KB, FL,
               V, HB, HE, HP, PK, G1a, G2a, G1b, G2b, G1d, G2d, Ccat, cr, wr, cst, pqs,
               ld_sem, own_sem, h0_s, h0_r, v0_s, v0_r, h1_s, h1_r, v1_s, v1_r, v_s, v_r, hm_s, hm_r,
               a1_s, a1_r, a2_s, a2_r, b1_s, b1_r, b2_s, b2_r, d1_s, d1_r, d2_s, d2_r, out_sem):
    sx = lax.axis_index("sx")
    sy = lax.axis_index("sy")
    left, right = {"sy": sy - 1}, {"sy": sy + 1}
    has_left, has_right = sy > 0, sy < LAST
    has = (sx > 0, sx < LAST)
    near = lax.rem(sx, 2)
    inner = (sx > 0) & (sx < LAST)

    def rc(src, dst, s, q, dev):
        return pltpu.make_async_remote_copy(src, dst, s, q, device_id=dev, device_id_type=MESH)

    own = pl.ds(OWN, M)
    inv_cp = [pltpu.make_async_copy(inv_hbm.at[pl.ds(CHUNK * c, CHUNK)], stage.at[c], ld_sem.at[c]) for c in range(SIDE)]
    own_cp = [pltpu.make_async_copy(f_hbm.at[:, :, pl.ds(LANES * h, LANES)], S48.at[h, own, pl.ds(SUB, M)], own_sem.at[h]) for h in HALVES]
    each(own_cp, "start")
    each(inv_cp, "start")
    zrow = jnp.zeros((len(PIECES), OWN, WIDE, LANES), F32)
    S48[:, 0:OWN] = zrow
    S48[:, OWN + M:] = zrow
    zcol = jnp.zeros((len(PIECES), M, SUB, LANES), F32)
    S48[:, OWN:OWN + M, 0:SUB] = zcol
    S48[:, OWN:OWN + M, ME:] = zcol
    for b in (V, HB, HE, HP):
        b[...] = jnp.zeros(b.shape, F32)

    bar = pltpu.get_barrier_semaphore()
    for d in FAR:
        pl.semaphore_signal(bar, inc=1, device_id={"sx": lax.rem(sx + d, SIDE)}, device_id_type=MESH)
        pl.semaphore_signal(bar, inc=1, device_id={"sy": lax.rem(sy + d, SIDE)}, device_id_type=MESH)
    pl.semaphore_wait(bar, 2 * LAST)

    def first_copies(G1, s, q):
        return [rc(G1.at[sy], G1.at[sy], s.at[d - 1], q.at[d - 1], {"sy": lax.rem(sy + d, SIDE)}) for d in FAR]

    def second_copies(src, G2, s, q):
        return [rc(src, G2.at[sx], s.at[d - 1], q.at[d - 1], {"sx": lax.rem(sx + d, SIDE)}) for d in FAR]

    a1 = first_copies(G1a, a1_s, a1_r)
    a2 = second_copies(G1a, G2a, a2_s, a2_r)
    b1 = first_copies(G1b, b1_s, b1_r)
    b2 = second_copies(G2b.at[sx], G2b, b2_s, b2_r)
    d1 = first_copies(G1d, d1_s, d1_r)
    d2 = second_copies(G2d.at[sx], G2d, d2_s, d2_r)
    mine_y, mine_x = pl.ds(sy, 1), pl.ds(sx, 1)

    def half_sum(G1, G2, one, two):
        each(one, "wait")
        G2[mine_x] = jnp.sum(G1[...], axis=0, keepdims=True)
        each(two, "start")

    def full_sum(G2, two):
        each(two, "wait")
        return jnp.sum(G2[...], axis=0)

    G1b[mine_y] = jnp.broadcast_to(cnt_ref[...], (1, 2, SUB, LANES))
    each(b1, "start")

    def halos(slabs, hs, hr, vs, vr):
        h = [rc(S48.at[slabs, own, pl.ds(SUB, SUB)], S48.at[slabs, own, pl.ds(ME, SUB)], hs.at[0], hr.at[0], left),
             rc(S48.at[slabs, own, pl.ds(M, SUB)], S48.at[slabs, own, pl.ds(0, SUB)], hs.at[1], hr.at[1], right)]
        v = [rc(S48.at[slabs, pl.ds(OWN, OWN)], S48.at[slabs, pl.ds(OWN + M, OWN)], vs.at[0], vr.at[1], {"sx": sx - 1}),
             rc(S48.at[slabs, pl.ds(M, OWN)], S48.at[slabs, pl.ds(0, OWN)], vs.at[1], vr.at[0], {"sx": sx + 1})]
        v_in = [rc(S48.at[slabs, pl.ds(0, OWN)], S48.at[slabs, pl.ds(0, OWN)], vs.at[e], vr.at[e], left) for e in HALVES]
        return h, v, v_in
    f_h, f_v, f_in = halos(pl.ds(0, 2), h0_s, h0_r, v0_s, v0_r)
    k_h, k_v, k_in = halos(pl.ds(2, 1), h1_s, h1_r, v1_s, v1_r)

    def go(pair):
        pl.when(has_left)(pair[0].start)
        pl.when(has_right)(pair[1].start)

    def come(pair):
        pl.when(has_right)(pair[0].wait_recv)
        pl.when(has_left)(pair[1].wait_recv)

    def gone(pair):
        pl.when(has_left)(pair[0].wait_send)
        pl.when(has_right)(pair[1].wait_send)

    def up_down(pair, what):
        for e in HALVES:
            pl.when(has[e])(getattr(pair[e], what))
    each(own_cp, "wait")
    go(f_h)

    slot = mult(KMAX * (sx * SIDE + sy), KMAX)
    FL[...] = jnp.zeros(FL.shape, F32)
    FL[pl.ds(slot, KMAX), 0:M * M] = own_ref[...]
    for k in range(SUB):
        S48[2, OWN + D * k:OWN + D * (k + 1), SUB:ME] = FL[:, lanes(k)].T.reshape(D, M, LANES)
    go(k_h)

    def shifted(v, k=D):
        return pltpu.roll(v, WIDE - k, 0)[0:ME]
    lane_of = lax.broadcasted_iota(jnp.int32, (WIDE, LANES), 1)
    last_slot = lane_of % KMAX == KMAX - 1

    def basis_of(v):
        return jnp.where(last_slot[0:ME], 0.0, v)

    def own_rows(i, c):
        mine = S48[2, i + 1, SUB:ME]
        mine = jnp.concatenate([mine, jnp.zeros((BT, LANES), F32)], axis=0)
        W5[0, i] = basis_of(pltpu.roll(mine, D, 0)[0:ME])
        return c
    for i in list(range(D)) + list(range(D + M, ME)):
        W5[0, i] = jnp.zeros((ME, LANES), F32)
    lax.fori_loop(D, D + M, own_rows, 0)
    flat = W5[0].reshape(NE, LANES)
    for k in range(NP // LANES):
        blk = flat[LANES * k:LANES * (k + 1)]
        if blk.shape[0] < LANES:
            blk = jnp.concatenate([blk, jnp.zeros_like(blk)], axis=0)
        FL[:, lanes(k)] = blk.T
    restrict = FL[pl.ds(slot, KMAX), 0:NE]
    restrict = jnp.concatenate([restrict, jnp.zeros_like(restrict)], axis=0)

    for b in (p, z, r, l, x, T):
        def zero(i, c, b=b):
            b[:, pl.ds(i, 1)] = jnp.zeros((2, 1, ME, LANES), F32)
            return c
        lax.fori_loop(0, b.shape[1], zero, 0)
    Xr[...] = jnp.zeros(Xr.shape, BF16)
    for b in (cr, wr, cst, pqs, nrm_ref):
        b[...] = jnp.zeros(b.shape, F32)

    def put_l(v, rows):
        one, two, three = split3(v)
        rest = []
        for k, piece in enumerate((one, two, three)):
            L[rows, KM * k:KM * (k + 1)] = piece[:, 0:KM]
            rest.append(piece[:, KM:].astype(F32))
        twice = jnp.concatenate(rest[0:2], axis=1).astype(BF16)
        Lr[rows, lanes(0)] = twice
        Lr[rows, lanes(1)] = twice
        Lr[rows, lanes(2)] = jnp.concatenate([rest[0], rest[2]], axis=1).astype(BF16)
        Lr[rows, lanes(LAST)] = jnp.zeros(twice.shape, BF16)

    for at in (0, LAST * CHUNK + BT):
        put_l(restrict, pl.ds(at, BT))
    half_sum(G1b, G2b, b1, b2)

    def split_inv(c):
        inv_cp[c].wait()

        def body(k, carry):
            put_l(stage[c, pl.ds(mult(BT * k), BT), :], pl.ds(mult(CHUNK * c + BT * (c // LAST + 1) + BT * k), BT))
            return carry
        lax.fori_loop(0, CHUNK // BT, body, 0)

    split_inv(0)
    split_inv(1)
    come(f_h)
    gone(f_h)
    up_down(f_v, "start")
    split_inv(2)
    split_inv(LAST)

    def dot(a, b):
        return jnp.dot(a, b, preferred_element_type=F32)

    def dot_pieces(lhs, v):
        y1, y2, y3 = split3(v)
        total = 0.0
        for n, two in enumerate(((y1, y1), (y2, y2), (y3, y1))):
            total = total + dot(lhs(LANES * (n // 2)), jnp.concatenate(two, axis=0))
        return total

    cnt = full_sum(G2b, b2)[0]
    lane = lax.broadcasted_iota(jnp.int32, (SUB, LANES), 1)
    starts = cnt
    for d in (KMAX, 2 * KMAX, D * KMAX, SUB * KMAX):
        starts = starts + jnp.where(lane >= d, pltpu.roll(starts, d, 1), 0.0)
    starts = starts - cnt
    col = (lane % KMAX).astype(F32)
    target = jnp.where(col < cnt, starts + col, -1.0)
    half = cinv_ref.shape[0]
    pick = jnp.where(lax.broadcasted_iota(jnp.int32, (half, LANES), 0).astype(F32) == row(target, 0), 1.0, 0.0)

    def rhs_of(parts):
        v = jnp.concatenate(parts + [jnp.zeros_like(parts[0])], axis=0)
        return v.astype(BF16)

    def lhs_of(parts):
        v = jnp.concatenate(parts + [jnp.zeros_like(parts[0])], axis=1)
        return v.astype(BF16)

    def as_f32(v):
        return [piece.astype(F32) for piece in split3(v)]
    spread = dot(lhs_of(as_f32(cinv_ref[...])), rhs_of([pick] * len(PIECES)))
    spread = dot(lhs_of([pick.T] * len(PIECES)), rhs_of(as_f32(spread)))

    def put_middle(ref, rows, v):
        for k, piece in zip((1, 0, 2), split3(v)):
            ref[rows, lanes(k)] = piece
    put_middle(Ccat, pl.ds(0, LANES), spread)

    come(k_h)
    gone(k_h)
    up_down(k_v, "start")
    up_down(f_v, "wait_send")
    up_down(f_in, "wait_recv")

    jcol = lax.broadcasted_iota(jnp.int32, (ME, LANES), 0)
    gj = sy * M + jcol - D
    in_col = (gj >= 0) & (gj < GRID)

    def kappa_rows(i, c):
        KB[i] = jnp.broadcast_to(jnp.sum(jnp.where(last_slot, S48[2, i], 0.0), axis=1, keepdims=True), (WIDE, LANES))
        return c

    def weights(i, c):
        gi = sx * M + i - D
        ok = in_col & (gi >= 0) & (gi < GRID)
        here = KB[i + 1]
        kc = shifted(here)

        def pair(other, inside):
            both = ok & inside
            w = jnp.where(both, 2.0 * kc * other / jnp.where(both, kc + other, 1.0), 0.0)
            return w, jnp.where(ok & jnp.logical_not(inside), kc, w)
        edges = (pair(shifted(KB[i]), ok & (gi > 0)), pair(shifted(KB[i + 2]), ok & (gi < GRID - 1)),
                 pair(shifted(here, D - 1), gj > 0), pair(shifted(here, D + 1), gj < GRID - 1))
        total = 0.0
        for k, (w, d) in enumerate(edges):
            W5[k, i] = w
            total = total + d
        W5[SIDE, i] = total
        return c

    def pair_of(two, k):
        return jnp.concatenate(two, axis=0), pl.ds(mult(2 * ME * k), 2 * ME)

    def basis_rows(k, c):
        v, rows = pair_of([basis_of(shifted(S48[2, 2 * k + j])) for j in HALVES], k)
        put_middle(Ecat, rows, v)
        return c
    def geometry():
        up_down(k_v, "wait_send")
        up_down(k_in, "wait_recv")
        lax.fori_loop(0, M + 2 * OWN, kappa_rows, 0)
        lax.fori_loop(0, ME, weights, 0)
        for i in range(ME):
            RE[0, i:i + 1] = S48[2, i + 1, D - 1:D]
            RE[1, i:i + 1] = S48[2, i + 1, LOW:LOW + 1]
        lax.fori_loop(0, LOW // 2 - 1, basis_rows, 0)
        v, rows = pair_of([basis_of(RE[j]) for j in HALVES], LOW // 2 - 1)
        put_middle(Ecat, rows, v)

    def put_x(two, h, k):
        v, rows = pair_of(two, k)
        pieces = split3(v)
        if isinstance(k, int) and k == ME // 2 - 1:
            n = KM - 2 * ME * k
            for j, piece in enumerate(pieces):
                X[j, KM - n:KM, lanes(h)] = piece[0:n]
            for slot, j in enumerate((0, 0, 1, 1, 2, 0)):
                Xr[REM * slot:REM * (slot + 1), lanes(h)] = pieces[j][n:]
        else:
            for j, piece in enumerate(pieces):
                X[j, rows, lanes(h)] = piece

    def first_rows(k, c):
        for h in HALVES:
            two = [shifted(S48[h, 2 * k + 1 + j]) for j in HALVES]
            for j in HALVES:
                Q[h, 2 * k + 1 + j] = two[j]
            put_x(two, h, k)
        return c
    lax.fori_loop(0, ME // 2 - 1, first_rows, 0)
    first_rows(ME // 2 - 1, 0)

    colf = jnp.where((jcol >= D) & (jcol < D + M), 1.0, 0.0)
    sub8 = lax.broadcasted_iota(jnp.int32, (SUB, LANES), 0)
    zero = jnp.zeros((ME, LANES), F32)

    def product(start, n):
        first = NA
        outs = []
        for at, size in ((0, first), (first, n - first)):
            rows = pl.ds(mult(start + at), size)
            total = dot(Lr[rows, :], Xr[...])
            for j in PIECES:
                for i in PIECES[:len(PIECES) - j]:
                    total = total + dot(L[rows, KM * i:KM * (i + 1)], X[j])
            outs.append(total)
        return outs

    def put_t(outs, c):
        at = 0
        for v in outs:
            while v.shape[0]:
                top, off = 1 + ROWS * c + at // ME, at % ME
                n = min(ME - off, v.shape[0]) if off or v.shape[0] < ME else v.shape[0] // ME * ME
                whole = max(n // ME, 1)
                for h in HALVES:
                    T[h, pl.ds(top, whole), off:off + n // whole] = v[0:n, lanes(h)].reshape(whole, n // whole, LANES)
                v, at = v[n:], at + n

    def v_copy(e):
        return rc(T.at[:, pl.ds(1 + (M - 1) * e, STRIP)], V.at[1 - e], v_s.at[e], v_r.at[1 - e], {"sx": sx - 1 + 2 * e})

    def step(m, carry):
        par = lax.rem(m, 2)

        def side(n, src, dst):
            return [rc(src[j], dst.at[par, 1 - j], hm_s.at[par, j, n], hm_r.at[par, 1 - j, n], (left, right)[j]) for j in HALVES]

        def cols(ref, lo, n):
            return [ref.at[:, pl.ds(lo, n), pl.ds(M * j, SUB)] for j in HALVES]

        mids = [side(n, cols(T, EDGE + ROWS * n, ROWS), HB.at[:, :, n]) for n in HALVES]
        edges = [side(2 + e, cols(TE, EDGE * e, EDGE), HE.at[:, :, e]) for e in (near, 1 - near)]
        ring = side(SIDE, (PK.at[0], PK.at[1]), HP)
        everything = mids + edges + [ring]
        v_near, v_far = v_copy(near), v_copy(1 - near)

        def edge(e, pair):
            for h in HALVES:
                TE[h, pl.ds((EDGE + 2) * e, STRIP)] = T[h, pl.ds((M + 1) * e, STRIP)] + V[e, h]
                TE[h, pl.ds(STRIP + 2 * e, 2)] = T[h, pl.ds(STRIP + 2 * EDGE * e, 2)]
            go(pair)

        first = m == 0
        c0, c3 = LAST * near, LAST * (1 - near)
        for h in HALVES:
            G1d[mine_y, h] = pqs[h][None]
        each(d1, "start")
        out = product((LAST * CHUNK + BT) * near, CHUNK + BT)
        put_t([out[0][BT:], out[1]], c0)
        for h in HALVES:
            G1a[mine_y, h] = out[0][0:SUB, lanes(h)][None]
        each(a1, "start")
        pl.when(inner)(v_near.start)
        pl.when(jnp.logical_not(inner))(lambda: edge(near, edges[0]))
        put_t(product(BT + CHUNK, CHUNK), 1)
        go(mids[0])
        half_sum(G1d, G2d, d1, d2)
        put_t(product(BT + 2 * CHUNK, CHUNK), 2)
        go(mids[1])
        each(a1, "wait")
        each(a2, "start")

        pq = full_sum(G2d, d2)
        alpha = [jnp.where(first, -1.0, row(cst[0, h], 0) / row(pq[h], 0)) for h in HALVES]
        tot = [[zero, zero] for h in HALVES]

        def update(c, inside):
            for h in HALVES:
                for k in range(ROWS):
                    i = 1 + ROWS * c + k
                    rn = r[h, i] - alpha[h] * Q[h, i]
                    ln = l[h, i] - alpha[h] * T[h, i]
                    r[h, i] = rn
                    l[h, i] = ln
                    x[h, i] = x[h, i] + alpha[h] * p[h, i]
                    w = colf if inside else jnp.where((i >= OWN) & (i < OWN + M), 1.0, 0.0) * colf
                    tot[h][0] = tot[h][0] + rn * ln
                    tot[h][1] = tot[h][1] + w * (rn * rn)

        out = product(BT + (LAST * CHUNK + BT) * (1 - near), CHUNK)
        update(c0, False)
        update(1, True)
        update(2, True)
        put_t(out, c3)
        v_far.start()
        G2a[mine_x] = G1a[...][None]
        each(a2, "wait_send")
        update(c3, False)
        for h in HALVES:
            G1b[mine_y, h] = jnp.where(sub8 == 0, colsum(tot[h][0]), jnp.where(sub8 == 1, colsum(tot[h][1]), 0.0))[None]
        each(b1, "start")

        @pl.when(inner)
        def _():
            v_near.wait_send()
            rc(T.at[:, pl.ds(1, STRIP)], V.at[near], v_s.at[near], v_r.at[near], left).wait_recv()
            edge(near, edges[0])

        v_far.wait_send()
        rc(T.at[:, pl.ds(1, STRIP)], V.at[1 - near], v_s.at[near], v_r.at[1 - near], left).wait_recv()
        edge(1 - near, edges[1])
        for h in HALVES:
            for i in range(1, ME + 1):
                src, k = (TE, i) if i < EDGE else ((T, i) if i < M - 1 else (TE, i - 2 * ROWS))
                PK[0, h, i - 1:i] = src[h, k, SUB:SUB + 1]
                PK[1, h, i - 1:i] = src[h, k, M - 1:M]
        go(ring)

        pl.when(first)(geometry)
        each(a2, "wait_recv")
        cq = jnp.concatenate([G2a[:, :, h].reshape(LANES, LANES) for h in HALVES], axis=1)
        yq = dot_pieces(lambda at: Ccat[:, at:at + TILE], cq)
        rzc = []
        for h in HALVES:
            cr[h] = cr[h] - alpha[h] * cq[:, lanes(h)]
            wr[h] = wr[h] - alpha[h] * yq[:, lanes(h)]
            rzc.append(colsum(cr[h] * wr[h]))
        n = LOW // 2
        for part in HALVES:
            o = dot_pieces(lambda at: Ecat[ME * n * part:ME * n * (part + 1), at:at + TILE], yq)
            for h in HALVES:
                Ey[h, n * part:n * (part + 1)] = o[:, lanes(h)].reshape(n, ME, LANES)

        half_sum(G1b, G2b, b1, b2)
        got = full_sum(G2b, b2)
        beta = []
        for h in HALVES:
            rzn = row(got[h], 0) + rzc[h]
            rr = row(got[h], 1)
            beta.append(jnp.where(first, 0.0, rzn / row(cst[0, h], 0)))
            ff = jnp.where(first, jnp.sqrt(rr), row(cst[1, h], 0))
            cst[0, h] = wide(rzn)
            cst[1, h] = wide(ff)
            nrm_ref[:, lanes(h)] = jnp.where(sub8 == m - 1, jnp.sqrt(rr) / ff, nrm_ref[:, lanes(h)])

        for pair in everything:
            come(pair)

        def renew(i, u):
            for h in HALVES:
                zn = z[h, i] - alpha[h] * (u[h] + Ey[h, i])
                z[h, i] = zn
                p[h, i] = zn + beta[h] * p[h, i]

        def sides(b, buf, n, h, k):
            return jnp.concatenate([b[0:SUB] + buf[par, 0, n, h, k], b[SUB:M], b[M:] + buf[par, 1, n, h, k]], axis=0)

        def mid_rows(k, c):
            for n in HALVES:
                i = EDGE + ROWS * n + k
                renew(i, [sides(T[h, i], HB, n, h, k) for h in HALVES])
            return c
        lax.fori_loop(0, ROWS, mid_rows, 0)

        def edge_rows(k, c):
            for n in HALVES:
                renew((M - 1) * n + k, [sides(TE[h, EDGE * n + k], HE, n, h, k) for h in HALVES])
            return c
        lax.fori_loop(0, EDGE, edge_rows, 0)
        for j in HALVES:
            renew(LOW - 2 + j, [HP[par, j, h] for h in HALVES])

        def apply_rows(g, car):
            sums = list(car)
            rings = [[p[h, LOW - 2 + j, pl.ds(mult(SUB * g, SUB), SUB), :] for j in HALVES] for h in HALVES]
            rows = [[], []]
            for k in range(SUB):
                i = SUB * g + k
                w = [W5[j, i] for j in range(SIDE + 1)]
                own_f = jnp.where((i >= D) & (i < D + M), 1.0, 0.0) * colf
                for h in HALVES:
                    c = p[h, i + 1]
                    west = jnp.where(jcol == 0, row(rings[h][0], k), pltpu.roll(c, 1, 0))
                    east = jnp.where(jcol == ME - 1, row(rings[h][1], k), pltpu.roll(c, ME - 1, 0))
                    q = w[SIDE] * c
                    for j, other in enumerate((p[h, i], p[h, i + 2], west, east)):
                        q = q - w[j] * other
                    Q[h, i + 1] = q
                    sums[h] = sums[h] + own_f * (c * q)
                    rows[h].append(q)
                    if len(rows[h]) == 2:
                        put_x(rows[h], h, D * g + k // 2)
                        rows[h] = []
            return tuple(sums)
        car = lax.fori_loop(0, ME // SUB - 1, apply_rows, (zero, zero))
        car = apply_rows(ME // SUB - 1, car)
        for h in HALVES:
            pqs[h] = wide(colsum(car[h]))

        for pair in everything:
            gone(pair)
        return carry

    lax.fori_loop(0, ITERS, step, 0)

    for h in HALVES:
        G1d[mine_y, h] = pqs[h][None]
    each(d1, "start")
    half_sum(G1d, G2d, d1, d2)
    pq = full_sum(G2d, d2)
    alpha = [row(cst[0, h], 0) / row(pq[h], 0) for h in HALVES]

    def finish(i, car):
        res = []
        for h in HALVES:
            rn = r[h, i] - alpha[h] * Q[h, i]
            res.append(car[h] + colf * (rn * rn))
            xn = x[h, i] + alpha[h] * p[h, i]
            T[h, i, 0:M] = pltpu.roll(jnp.concatenate([xn, xn[0:SUB]], axis=0), WIDE - D, 0)[0:M]
        return tuple(res)
    rr = lax.fori_loop(OWN, OWN + M, finish, (zero, zero))
    out_cp = [pltpu.make_async_copy(T.at[h, own, pl.ds(0, M)], x_hbm.at[:, :, pl.ds(LANES * h, LANES)], out_sem.at[h]) for h in HALVES]
    each(out_cp, "start")
    for h in HALVES:
        G1b[mine_y, h] = wide(colsum(rr[h]))[None]
    each(b1, "start")
    half_sum(G1b, G2b, b1, b2)
    got = full_sum(G2b, b2)
    for h in HALVES:
        nrm_ref[:, lanes(h)] = jnp.where(sub8 == ITERS - 1, jnp.sqrt(row(got[h], 0)) / row(cst[1, h], 0), nrm_ref[:, lanes(h)])
    each(out_cp, "wait")


def solution(mesh):
    def dma(*shape):
        return pltpu.SemaphoreType.DMA(shape)

    def vm(*shape, dtype=F32):
        return pltpu.VMEM(shape, dtype)

    field = vm(2, LOW, ME, LANES)
    strips = [vm(2, 2, 2, 2, n, SUB, LANES) for n in (ROWS, EDGE)]
    gathers = [vm(SIDE, 2, SUB, LANES), vm(SIDE, SIDE, 2, SUB, LANES)] + [vm(SIDE, 2, SUB, LANES)] * SIDE
    scratch = [
        vm(len(PIECES), M + 2 * OWN, WIDE, LANES), vm(NL, KM * len(PIECES), dtype=BF16), vm(NL, 2 * TILE, dtype=BF16),
        vm(SIDE, CHUNK, NE), vm(len(PIECES), KM, TILE, dtype=BF16), vm(2 * TILE, TILE, dtype=BF16),
        field, vm(2, 2 * EDGE, ME, LANES), field, field, field, field, field, field, field,
        vm(SIDE + 1, ME, ME, LANES), vm(LOW * ME, LANES * len(PIECES), dtype=BF16), vm(2, ME, LANES), vm(M + 2 * OWN, WIDE, LANES), vm(LANES, NP),
        vm(2, 2, STRIP, ME, LANES), *strips, vm(2, 2, 2, ME, LANES), vm(2, 2, ME, LANES), *gathers,
        vm(LANES, LANES * len(PIECES), dtype=BF16), vm(2, LANES, LANES), vm(2, LANES, LANES), vm(2, 2, SUB, LANES),
        vm(2, SUB, LANES), dma(SIDE), dma(2), *[dma(2)] * 10, *[dma(2, 2, SIDE + 1)] * 2, *[dma(LAST)] * 12, dma(2),
    ]
    any_spec = pl.BlockSpec(memory_space=pl.ANY)
    vmem_spec = pl.BlockSpec(memory_space=pltpu.VMEM)

    def body(forcing, kappa, local_inv, coarse_basis, coarse_counts, coarse_inv):
        index = lax.axis_index("sx") * SIDE + lax.axis_index("sy")
        own = jnp.concatenate([coarse_basis[0].T[:KMAX - 1], kappa.reshape(1, M * M)], axis=0)
        mine = jnp.arange(LANES) // KMAX == index
        cnt = jnp.broadcast_to(jnp.where(mine, coarse_counts.astype(F32), 0.0)[None, :], (SUB, LANES))
        return pl.pallas_call(
            solve_kernel,
            out_shape=(jax.ShapeDtypeStruct((M, M, 2 * LANES), F32), jax.ShapeDtypeStruct((ITERS, 2 * LANES), F32)),
            in_specs=[any_spec] * 2 + [vmem_spec] * len(PIECES),
            out_specs=(any_spec, vmem_spec),
            scratch_shapes=scratch,
            compiler_params=pltpu.CompilerParams(collective_id=0, has_side_effects=True, vmem_limit_bytes=67043328),
        )(forcing, local_inv[0], own, coarse_inv, cnt)

    cell_spec = P(("batch", "sx"), "sy", None)
    sub_spec = P(("batch", "sx", "sy"), None, None)
    return jax.shard_map(body, mesh=mesh, in_specs=(cell_spec, P(("batch", "sx"), "sy"), sub_spec, sub_spec, P(("batch", "sx", "sy")), P("batch", None)), out_specs=(cell_spec, P("batch", None)), check_vma=False)
```

```python
import jax
import jax.numpy as jnp
from jax import lax
from jax.experimental import pallas as pl
from jax.experimental.pallas import tpu as pltpu
from jax.sharding import PartitionSpec as P

ITERS = 8
M = 32
D = 4
ME = M + 2 * D
NE = ME * ME
SUB = 8
LANES = 128
TILE = 256
KT = NE // TILE
KM = KT * TILE
REM = NE - KM
ROWS = 10
CHUNK = ROWS * ME
NP = NE + REM
NA = 208
BT = 16
NL = NE + 2 * BT
KMAX = 8
GRID = 128
LOW = M + SUB + D
WIDE = M + 2 * SUB
OWN = D + 1
STRIP = 9
EDGE = STRIP + 2
MESH = pl.DeviceIdType.MESH
HI = lax.Precision.HIGHEST
F32 = jnp.float32
BF16 = jnp.bfloat16
HALVES = (0, 1)
PIECES = (0, 1, 2)
FAR = (1, 2, 3)
LAST = FAR[-1]
SIDE = FAR[-1] + 1


def lanes(h):
    return slice(LANES * h, LANES * (h + 1))


def tile(k):
    return slice(TILE * k, TILE * (k + 1))


def mult(v, n=BT):
    return v if isinstance(v, int) else pl.multiple_of(v, n)


def row(v, k):
    return v[k:k + 1]


def wide(v):
    return jnp.broadcast_to(v, (SUB, LANES))


def colsum(v):
    return jnp.sum(v, axis=0, keepdims=True)


def each(copies, what):
    for c in copies:
        getattr(c, what)()


def split3(v):
    hi = v.astype(BF16)
    rest = v - hi.astype(F32)
    mid = rest.astype(BF16)
    low = (rest - mid.astype(F32)).astype(BF16)
    return hi, mid, low


def solve_kernel(f_hbm, inv_hbm, own_ref, cinv_ref, cnt_ref, x_hbm, nrm_ref,
                 S48, L, Lr, stage, X, Xr, T, TE, z, p, r, l, x, Q, Ey, W5, Ecat, RE, KB, FL,
               V, HB, HE, HP, PK, G1a, G2a, Gb, Gd, Ccat, cr, wr, cst, pqs,
               ld_sem, own_sem, h0_s, h0_r, v0_s, v0_r, h1_s, h1_r, v1_s, v1_r, v_s, v_r, hm_s, hm_r,
               a1_s, a1_r, a2_s, a2_r, b_s, b_r, d_s, d_r, out_sem):
    sx = lax.axis_index("sx")
    sy = lax.axis_index("sy")
    left, right = {"sy": sy - 1}, {"sy": sy + 1}
    has_left, has_right = sy > 0, sy < LAST
    has = (sx > 0, sx < LAST)
    near = lax.rem(sx, 2)
    inner = (sx > 0) & (sx < LAST)

    def rc(src, dst, s, q, dev):
        return pltpu.make_async_remote_copy(src, dst, s, q, device_id=dev, device_id_type=MESH)

    own = pl.ds(OWN, M)
    inv_cp = [pltpu.make_async_copy(inv_hbm.at[pl.ds(CHUNK * c, CHUNK)], stage.at[c], ld_sem.at[c]) for c in range(SIDE)]
    own_cp = [pltpu.make_async_copy(f_hbm.at[:, :, pl.ds(LANES * h, LANES)], S48.at[h, own, pl.ds(SUB, M)], own_sem.at[h]) for h in HALVES]
    each(own_cp, "start")
    each(inv_cp, "start")
    zrow = jnp.zeros((len(PIECES), OWN, WIDE, LANES), F32)
    S48[:, 0:OWN] = zrow
    S48[:, OWN + M:] = zrow
    zcol = jnp.zeros((len(PIECES), M, SUB, LANES), F32)
    S48[:, OWN:OWN + M, 0:SUB] = zcol
    S48[:, OWN:OWN + M, ME:] = zcol
    for b in (V, HB, HE, HP):
        b[...] = jnp.zeros(b.shape, F32)

    bar = pltpu.get_barrier_semaphore()
    peers = [{"sx": lax.rem(sx + k // SIDE, SIDE), "sy": lax.rem(sy + k % SIDE, SIDE)} for k in range(1, SIDE * SIDE)]
    for peer in peers:
        pl.semaphore_signal(bar, inc=1, device_id=peer, device_id_type=MESH)
    pl.semaphore_wait(bar, len(peers))

    def first_copies(G1, s, q):
        return [rc(G1.at[sy], G1.at[sy], s.at[d - 1], q.at[d - 1], {"sy": lax.rem(sy + d, SIDE)}) for d in FAR]

    a1 = first_copies(G1a, a1_s, a1_r)
    mine_y, mine_x = pl.ds(sy, 1), pl.ds(sx, 1)

    def gather(G, s, q):
        me = SIDE * sx + sy
        return me, [rc(G.at[me], G.at[me], s.at[k], q.at[k], peer) for k, peer in enumerate(peers)]
    sub4 = lax.broadcasted_iota(jnp.int32, (SIDE, LANES), 0)

    def send_rows(G, s, q, rows):
        me, copies = gather(G, s, q)
        v = jnp.zeros((SIDE, LANES), F32)
        for k, one in enumerate(rows):
            v = jnp.where(sub4 == k, one, v)
        G[pl.ds(me, 1)] = v[None]
        each(copies, "start")

    def full_sum(G, s, q):
        each(gather(G, s, q)[1], "wait")
        return jnp.sum(G[...], axis=0)

    send_rows(Gb, b_s, b_r, [row(cnt_ref[...], 0)])

    def halos(slabs, hs, hr, vs, vr):
        h = [rc(S48.at[slabs, own, pl.ds(SUB, SUB)], S48.at[slabs, own, pl.ds(ME, SUB)], hs.at[0], hr.at[0], left),
             rc(S48.at[slabs, own, pl.ds(M, SUB)], S48.at[slabs, own, pl.ds(0, SUB)], hs.at[1], hr.at[1], right)]
        v = [rc(S48.at[slabs, pl.ds(OWN, OWN)], S48.at[slabs, pl.ds(OWN + M, OWN)], vs.at[0], vr.at[1], {"sx": sx - 1}),
             rc(S48.at[slabs, pl.ds(M, OWN)], S48.at[slabs, pl.ds(0, OWN)], vs.at[1], vr.at[0], {"sx": sx + 1})]
        v_in = [rc(S48.at[slabs, pl.ds(0, OWN)], S48.at[slabs, pl.ds(0, OWN)], vs.at[e], vr.at[e], left) for e in HALVES]
        return h, v, v_in
    f_h, f_v, f_in = halos(pl.ds(0, 2), h0_s, h0_r, v0_s, v0_r)
    k_h, k_v, k_in = halos(pl.ds(2, 1), h1_s, h1_r, v1_s, v1_r)

    def go(pair):
        pl.when(has_left)(pair[0].start)
        pl.when(has_right)(pair[1].start)

    def come(pair):
        pl.when(has_right)(pair[0].wait_recv)
        pl.when(has_left)(pair[1].wait_recv)

    def gone(pair):
        pl.when(has_left)(pair[0].wait_send)
        pl.when(has_right)(pair[1].wait_send)

    def up_down(pair, what):
        for e in HALVES:
            pl.when(has[e])(getattr(pair[e], what))
    each(own_cp, "wait")
    go(f_h)

    slot = mult(KMAX * (sx * SIDE + sy), KMAX)
    FL[...] = jnp.zeros(FL.shape, F32)
    FL[pl.ds(slot, KMAX), 0:M * M] = own_ref[...]
    for k in range(SUB):
        S48[2, OWN + D * k:OWN + D * (k + 1), SUB:ME] = FL[:, lanes(k)].T.reshape(D, M, LANES)
    go(k_h)

    def shifted(v, k=D):
        return pltpu.roll(v, WIDE - k, 0)[0:ME]
    lane_of = lax.broadcasted_iota(jnp.int32, (WIDE, LANES), 1)
    last_slot = lane_of % KMAX == KMAX - 1

    def basis_of(v):
        return jnp.where(last_slot[0:ME], 0.0, v)

    def own_rows(i, c):
        mine = S48[2, i + 1, SUB:ME]
        mine = jnp.concatenate([mine, jnp.zeros((BT, LANES), F32)], axis=0)
        W5[0, i] = basis_of(pltpu.roll(mine, D, 0)[0:ME])
        return c
    for i in list(range(D)) + list(range(D + M, ME)):
        W5[0, i] = jnp.zeros((ME, LANES), F32)
    lax.fori_loop(D, D + M, own_rows, 0)
    flat = W5[0].reshape(NE, LANES)
    for k in range(NP // LANES):
        blk = flat[LANES * k:LANES * (k + 1)]
        if blk.shape[0] < LANES:
            blk = jnp.concatenate([blk, jnp.zeros_like(blk)], axis=0)
        FL[:, lanes(k)] = blk.T
    restrict = FL[pl.ds(slot, KMAX), 0:NE]
    restrict = jnp.concatenate([restrict, jnp.zeros_like(restrict)], axis=0)

    for b in (p, z, r, l, x, T):
        def zero(i, c, b=b):
            b[:, pl.ds(i, 1)] = jnp.zeros((2, 1, ME, LANES), F32)
            return c
        lax.fori_loop(0, b.shape[1], zero, 0)
    Xr[...] = jnp.zeros(Xr.shape, BF16)
    for b in (cr, wr, cst, pqs, nrm_ref):
        b[...] = jnp.zeros(b.shape, F32)

    def put_l(v, rows):
        one, two, three = split3(v)
        rest = []
        for k, piece in enumerate((one, two, three)):
            L[rows, KM * k:KM * (k + 1)] = piece[:, 0:KM]
            rest.append(piece[:, KM:].astype(F32))
        twice = jnp.concatenate(rest[0:2], axis=1).astype(BF16)
        Lr[rows, lanes(0)] = twice
        Lr[rows, lanes(1)] = twice
        Lr[rows, lanes(2)] = jnp.concatenate([rest[0], rest[2]], axis=1).astype(BF16)
        Lr[rows, lanes(LAST)] = jnp.zeros(twice.shape, BF16)

    for at in (0, LAST * CHUNK + BT):
        put_l(restrict, pl.ds(at, BT))

    def split_inv(c):
        inv_cp[c].wait()

        def body(k, carry):
            put_l(stage[c, pl.ds(mult(BT * k), BT), :], pl.ds(mult(CHUNK * c + BT * (c // LAST + 1) + BT * k), BT))
            return carry
        lax.fori_loop(0, CHUNK // BT, body, 0)

    split_inv(0)
    split_inv(1)
    come(f_h)
    gone(f_h)
    up_down(f_v, "start")
    split_inv(2)
    split_inv(LAST)

    def dot(a, b):
        return jnp.dot(a, b, preferred_element_type=F32)

    def dot_pieces(lhs, v):
        y1, y2, y3 = split3(v)
        total = 0.0
        for n, two in enumerate(((y1, y1), (y2, y2), (y3, y1))):
            total = total + dot(lhs(LANES * (n // 2)), jnp.concatenate(two, axis=0))
        return total

    cnt = wide(row(full_sum(Gb, b_s, b_r), 0))
    lane = lax.broadcasted_iota(jnp.int32, (SUB, LANES), 1)
    starts = cnt
    for d in (KMAX, 2 * KMAX, D * KMAX, SUB * KMAX):
        starts = starts + jnp.where(lane >= d, pltpu.roll(starts, d, 1), 0.0)
    starts = starts - cnt
    col = (lane % KMAX).astype(F32)
    target = jnp.where(col < cnt, starts + col, -1.0)
    half = cinv_ref.shape[0]
    pick = jnp.where(lax.broadcasted_iota(jnp.int32, (half, LANES), 0).astype(F32) == row(target, 0), 1.0, 0.0)

    def rhs_of(parts):
        v = jnp.concatenate(parts + [jnp.zeros_like(parts[0])], axis=0)
        return v.astype(BF16)

    def lhs_of(parts):
        v = jnp.concatenate(parts + [jnp.zeros_like(parts[0])], axis=1)
        return v.astype(BF16)

    def as_f32(v):
        return [piece.astype(F32) for piece in split3(v)]
    spread = dot(lhs_of(as_f32(cinv_ref[...])), rhs_of([pick] * len(PIECES)))
    spread = dot(lhs_of([pick.T] * len(PIECES)), rhs_of(as_f32(spread)))

    def put_middle(ref, rows, v):
        for k, piece in zip((1, 0, 2), split3(v)):
            ref[rows, lanes(k)] = piece
    put_middle(Ccat, pl.ds(0, LANES), spread)

    come(k_h)
    gone(k_h)
    up_down(k_v, "start")
    up_down(f_v, "wait_send")
    up_down(f_in, "wait_recv")

    jcol = lax.broadcasted_iota(jnp.int32, (ME, LANES), 0)
    gj = sy * M + jcol - D
    in_col = (gj >= 0) & (gj < GRID)

    def kappa_rows(i, c):
        KB[i] = jnp.broadcast_to(jnp.sum(jnp.where(last_slot, S48[2, i], 0.0), axis=1, keepdims=True), (WIDE, LANES))
        return c

    def weights(i, c):
        gi = sx * M + i - D
        ok = in_col & (gi >= 0) & (gi < GRID)
        here = KB[i + 1]
        kc = shifted(here)

        def pair(other, inside):
            both = ok & inside
            w = jnp.where(both, 2.0 * kc * other / jnp.where(both, kc + other, 1.0), 0.0)
            return w, jnp.where(ok & jnp.logical_not(inside), kc, w)
        edges = (pair(shifted(KB[i]), ok & (gi > 0)), pair(shifted(KB[i + 2]), ok & (gi < GRID - 1)),
                 pair(shifted(here, D - 1), gj > 0), pair(shifted(here, D + 1), gj < GRID - 1))
        total = 0.0
        for k, (w, d) in enumerate(edges):
            W5[k, i] = w
            total = total + d
        W5[SIDE, i] = total
        return c

    def pair_of(two, k):
        return jnp.concatenate(two, axis=0), pl.ds(mult(2 * ME * k), 2 * ME)

    def basis_rows(k, c):
        v, rows = pair_of([basis_of(shifted(S48[2, 2 * k + j])) for j in HALVES], k)
        put_middle(Ecat, rows, v)
        return c
    def geometry():
        up_down(k_v, "wait_send")
        up_down(k_in, "wait_recv")
        lax.fori_loop(0, M + 2 * OWN, kappa_rows, 0)
        lax.fori_loop(0, ME, weights, 0)
        for i in range(ME):
            RE[0, i:i + 1] = S48[2, i + 1, D - 1:D]
            RE[1, i:i + 1] = S48[2, i + 1, LOW:LOW + 1]
        lax.fori_loop(0, LOW // 2 - 1, basis_rows, 0)
        v, rows = pair_of([basis_of(RE[j]) for j in HALVES], LOW // 2 - 1)
        put_middle(Ecat, rows, v)

    def put_x(two, h, k):
        v, rows = pair_of(two, k)
        pieces = split3(v)
        if isinstance(k, int) and k == ME // 2 - 1:
            n = KM - 2 * ME * k
            for j, piece in enumerate(pieces):
                X[j, KM - n:KM, lanes(h)] = piece[0:n]
            for slot, j in enumerate((0, 0, 1, 1, 2, 0)):
                Xr[REM * slot:REM * (slot + 1), lanes(h)] = pieces[j][n:]
        else:
            for j, piece in enumerate(pieces):
                X[j, rows, lanes(h)] = piece

    def first_rows(k, c):
        for h in HALVES:
            two = [shifted(S48[h, 2 * k + 1 + j]) for j in HALVES]
            for j in HALVES:
                Q[h, 2 * k + 1 + j] = two[j]
            put_x(two, h, k)
        return c
    lax.fori_loop(0, ME // 2 - 1, first_rows, 0)
    first_rows(ME // 2 - 1, 0)

    colf = jnp.where((jcol >= D) & (jcol < D + M), 1.0, 0.0)
    sub8 = lax.broadcasted_iota(jnp.int32, (SUB, LANES), 0)
    zero = jnp.zeros((ME, LANES), F32)

    def product(start, n):
        first = NA
        outs = []
        for at, size in ((0, first), (first, n - first)):
            rows = pl.ds(mult(start + at), size)
            total = dot(Lr[rows, :], Xr[...])
            for j in PIECES:
                for i in PIECES[:len(PIECES) - j]:
                    total = total + dot(L[rows, KM * i:KM * (i + 1)], X[j])
            outs.append(total)
        return outs

    def put_t(outs, c):
        at = 0
        for v in outs:
            while v.shape[0]:
                top, off = 1 + ROWS * c + at // ME, at % ME
                n = min(ME - off, v.shape[0]) if off or v.shape[0] < ME else v.shape[0] // ME * ME
                whole = max(n // ME, 1)
                for h in HALVES:
                    T[h, pl.ds(top, whole), off:off + n // whole] = v[0:n, lanes(h)].reshape(whole, n // whole, LANES)
                v, at = v[n:], at + n

    def v_copy(e, par):
        return rc(T.at[:, pl.ds(1 + (M - 1) * e, STRIP)], V.at[par, 1 - e], v_s.at[e], v_r.at[par, 1 - e], {"sx": sx - 1 + 2 * e})

    def v_wait(e, par):
        v_copy(e, par).wait_send()
        rc(T.at[:, pl.ds(1, STRIP)], V.at[par, e], v_s.at[e], v_r.at[par, e], left).wait_recv()

    def step(m, carry):
        par = lax.rem(m, 2)

        def side(n, src, dst):
            return [rc(src[j], dst.at[par, 1 - j], hm_s.at[par, j, n], hm_r.at[par, 1 - j, n], (left, right)[j]) for j in HALVES]

        def cols(ref, lo, n):
            return [ref.at[:, pl.ds(lo, n), pl.ds(M * j, SUB)] for j in HALVES]

        mids = [side(n, cols(T, EDGE + ROWS * n, ROWS), HB.at[:, :, n]) for n in HALVES]
        edges = [side(2 + e, cols(TE, EDGE * e, EDGE), HE.at[:, :, e]) for e in (near, 1 - near)]
        rings = [side(SIDE + n, [PK.at[j, :, pl.ds(at, size)] for j in HALVES], HP.at[:, :, :, pl.ds(at, size)])
                 for n, (at, size) in enumerate(((mult(BT * (1 - near)), ME - BT), (mult((ME - BT) * near, SUB), BT)))]
        everything = mids + edges + rings
        v_near, v_far = v_copy(near, par), v_copy(1 - near, par)
        a2 = [rc(G1a, G2a.at[par, sx], a2_s.at[d - 1], a2_r.at[par, d - 1], {"sx": lax.rem(sx + d, SIDE)}) for d in FAR]

        def edge(e, pair):
            for h in HALVES:
                TE[h, pl.ds((EDGE + 2) * e, STRIP)] = T[h, pl.ds((M + 1) * e, STRIP)] + V[par, e, h]
                TE[h, pl.ds(STRIP + 2 * e, 2)] = T[h, pl.ds(STRIP + 2 * EDGE * e, 2)]
            go(pair)

        def ring_rows(pairs):
            for h in HALVES:
                for at, ref, k in pairs:
                    for j, lane in enumerate((SUB, M - 1)):
                        PK[j, h, at] = ref[h, k, lane:lane + 1]

        def ring_edge(e):
            for h in HALVES:
                for k in range(ROWS):
                    for j, lane in enumerate((SUB, M - 1)):
                        PK[j, h, pl.ds((M - 2) * e + k, 1)] = TE[h, pl.ds(ROWS * e + 1 + k, 1), lane:lane + 1].reshape(1, LANES)

        first = m == 0
        c_near, c_far = LAST * near, LAST * (1 - near)
        start = (LAST * CHUNK + BT) * near
        send_rows(Gd, d_s, d_r, [row(pqs[h], 0) for h in HALVES])
        out = product((LAST * CHUNK + BT) - start, CHUNK + BT)
        put_t([out[0][BT:], out[1]], c_far)
        for h in HALVES:
            G1a[mine_y, h] = out[0][0:SUB, lanes(h)][None]
        each(a1, "start")
        v_far.start()
        put_t(product(BT + start, CHUNK), c_near)
        pl.when(inner)(v_near.start)
        pl.when(jnp.logical_not(inner))(lambda: edge(near, edges[0]))
        v_wait(1 - near, par)
        edge(1 - near, edges[1])
        put_t(product(BT + CHUNK, CHUNK), 1)
        go(mids[0])
        each(a1, "wait")
        each(a2, "start")

        pq = full_sum(Gd, d_s, d_r)
        alpha = [jnp.where(first, -1.0, row(cst[0, h], 0) / row(pq, h)) for h in HALVES]

        tot = [[zero, zero] for h in HALVES]

        def update(c, inside):
            for h in HALVES:
                for k in range(ROWS):
                    i = 1 + ROWS * c + k
                    rn = r[h, i] - alpha[h] * Q[h, i]
                    ln = l[h, i] - alpha[h] * T[h, i]
                    r[h, i] = rn
                    l[h, i] = ln
                    x[h, i] = x[h, i] + alpha[h] * p[h, i]
                    w = colf if inside else jnp.where((i >= OWN) & (i < OWN + M), 1.0, 0.0) * colf
                    tot[h][0] = tot[h][0] + rn * ln
                    tot[h][1] = tot[h][1] + w * (rn * rn)

        out = product(BT + 2 * CHUNK, CHUNK)
        update(c_far, False)
        update(c_near, False)
        update(1, True)
        put_t(out, 2)
        go(mids[1])
        update(2, True)
        G2a[par, mine_x] = G1a[...][None]
        each(a2, "wait_send")
        send_rows(Gb, b_s, b_r, [colsum(v) for two in tot for v in two])
        ring_rows([(slice(i - 1, i), T, i) for i in range(EDGE, M - 1)])
        ring_edge(1 - near)
        go(rings[0])

        @pl.when(inner)
        def _():
            v_wait(near, par)
            edge(near, edges[0])
        ring_edge(near)
        go(rings[1])

        pl.when(first)(geometry)
        each(a2, "wait_recv")
        cq = jnp.concatenate([G2a[par, :, :, h].reshape(LANES, LANES) for h in HALVES], axis=1)
        yq = dot_pieces(lambda at: Ccat[:, at:at + TILE], cq)
        rzc = []
        for h in HALVES:
            cr[h] = cr[h] - alpha[h] * cq[:, lanes(h)]
            wr[h] = wr[h] - alpha[h] * yq[:, lanes(h)]
            rzc.append(colsum(cr[h] * wr[h]))
        n = LOW // 2
        for part in HALVES:
            o = dot_pieces(lambda at: Ecat[ME * n * part:ME * n * (part + 1), at:at + TILE], yq)
            for h in HALVES:
                Ey[h, n * part:n * (part + 1)] = o[:, lanes(h)].reshape(n, ME, LANES)

        got = full_sum(Gb, b_s, b_r)
        beta = []
        for h in HALVES:
            rzn = row(got, 2 * h) + rzc[h]
            rr = row(got, 2 * h + 1)
            beta.append(jnp.where(first, 0.0, rzn / row(cst[0, h], 0)))
            ff = jnp.where(first, jnp.sqrt(rr), row(cst[1, h], 0))
            cst[0, h] = wide(rzn)
            cst[1, h] = wide(ff)
            nrm_ref[:, lanes(h)] = jnp.where(sub8 == m - 1, jnp.sqrt(rr) / ff, nrm_ref[:, lanes(h)])

        for pair in everything:
            come(pair)

        def renew(i, u):
            for h in HALVES:
                zn = z[h, i] - alpha[h] * (u[h] + Ey[h, i])
                z[h, i] = zn
                p[h, i] = zn + beta[h] * p[h, i]

        def sides(b, buf, n, h, k):
            return jnp.concatenate([b[0:SUB] + buf[par, 0, n, h, k], b[SUB:M], b[M:] + buf[par, 1, n, h, k]], axis=0)

        def mid_rows(k, c):
            for n in HALVES:
                i = EDGE + ROWS * n + k
                renew(i, [sides(T[h, i], HB, n, h, k) for h in HALVES])
            return c
        lax.fori_loop(0, ROWS, mid_rows, 0)

        def edge_rows(k, c):
            for n in HALVES:
                renew((M - 1) * n + k, [sides(TE[h, EDGE * n + k], HE, n, h, k) for h in HALVES])
            return c
        lax.fori_loop(0, EDGE, edge_rows, 0)
        for j in HALVES:
            renew(LOW - 2 + j, [HP[par, j, h] for h in HALVES])

        def apply_rows(g, car):
            sums = list(car)
            rings = [[p[h, LOW - 2 + j, pl.ds(mult(SUB * g, SUB), SUB), :] for j in HALVES] for h in HALVES]
            rows = [[], []]
            for k in range(SUB):
                i = SUB * g + k
                w = [W5[j, i] for j in range(SIDE + 1)]
                own_f = jnp.where((i >= D) & (i < D + M), 1.0, 0.0) * colf
                for h in HALVES:
                    c = p[h, i + 1]
                    west = jnp.where(jcol == 0, row(rings[h][0], k), pltpu.roll(c, 1, 0))
                    east = jnp.where(jcol == ME - 1, row(rings[h][1], k), pltpu.roll(c, ME - 1, 0))
                    q = w[SIDE] * c
                    for j, other in enumerate((p[h, i], p[h, i + 2], west, east)):
                        q = q - w[j] * other
                    Q[h, i + 1] = q
                    sums[h] = sums[h] + own_f * (c * q)
                    rows[h].append(q)
                    if len(rows[h]) == 2:
                        put_x(rows[h], h, D * g + k // 2)
                        rows[h] = []
            return tuple(sums)
        car = lax.fori_loop(0, ME // SUB - 1, apply_rows, (zero, zero))
        car = apply_rows(ME // SUB - 1, car)
        for h in HALVES:
            pqs[h] = wide(colsum(car[h]))

        for pair in everything:
            gone(pair)
        return carry

    lax.fori_loop(0, ITERS, step, 0)

    send_rows(Gd, d_s, d_r, [row(pqs[h], 0) for h in HALVES])
    pq = full_sum(Gd, d_s, d_r)
    alpha = [row(cst[0, h], 0) / row(pq, h) for h in HALVES]

    def finish(i, car):
        res = []
        for h in HALVES:
            rn = r[h, i] - alpha[h] * Q[h, i]
            res.append(car[h] + colf * (rn * rn))
            xn = x[h, i] + alpha[h] * p[h, i]
            T[h, i, 0:M] = pltpu.roll(jnp.concatenate([xn, xn[0:SUB]], axis=0), WIDE - D, 0)[0:M]
        return tuple(res)
    rr = lax.fori_loop(OWN, OWN + M, finish, (zero, zero))
    out_cp = [pltpu.make_async_copy(T.at[h, own, pl.ds(0, M)], x_hbm.at[:, :, pl.ds(LANES * h, LANES)], out_sem.at[h]) for h in HALVES]
    each(out_cp, "start")
    send_rows(Gb, b_s, b_r, [colsum(v) for v in rr])
    got = full_sum(Gb, b_s, b_r)
    for h in HALVES:
        nrm_ref[:, lanes(h)] = jnp.where(sub8 == ITERS - 1, jnp.sqrt(row(got, h)) / row(cst[1, h], 0), nrm_ref[:, lanes(h)])
    each(out_cp, "wait")


def solution(mesh):
    def dma(*shape):
        return pltpu.SemaphoreType.DMA(shape)

    def vm(*shape, dtype=F32):
        return pltpu.VMEM(shape, dtype)

    field = vm(2, LOW, ME, LANES)
    strips = [vm(2, 2, 2, 2, n, SUB, LANES) for n in (ROWS, EDGE)]
    gathers = [vm(SIDE, 2, SUB, LANES), vm(2, SIDE, SIDE, 2, SUB, LANES)] + [vm(SIDE * SIDE, SIDE, LANES)] * 2
    scratch = [
        vm(len(PIECES), M + 2 * OWN, WIDE, LANES), vm(NL, KM * len(PIECES), dtype=BF16), vm(NL, 2 * TILE, dtype=BF16),
        vm(SIDE, CHUNK, NE), vm(len(PIECES), KM, TILE, dtype=BF16), vm(2 * TILE, TILE, dtype=BF16),
        field, vm(2, 2 * EDGE, ME, LANES), field, field, field, field, field, field, field,
        vm(SIDE + 1, ME, ME, LANES), vm(LOW * ME, LANES * len(PIECES), dtype=BF16), vm(2, ME, LANES), vm(M + 2 * OWN, WIDE, LANES), vm(LANES, NP),
        vm(2, 2, 2, STRIP, ME, LANES), *strips, vm(2, 2, 2, ME, LANES), vm(2, 2, ME, LANES), *gathers,
        vm(LANES, LANES * len(PIECES), dtype=BF16), vm(2, LANES, LANES), vm(2, LANES, LANES), vm(2, 2, SUB, LANES),
        vm(2, SUB, LANES), dma(SIDE), dma(2), *[dma(2)] * 9, dma(2, 2), *[dma(2, 2, SIDE + 2)] * 2,
        *[dma(LAST)] * 3, dma(2, LAST), *[dma(SIDE * SIDE - 1)] * 4, dma(2),
    ]
    any_spec = pl.BlockSpec(memory_space=pl.ANY)
    vmem_spec = pl.BlockSpec(memory_space=pltpu.VMEM)

    def body(forcing, kappa, local_inv, coarse_basis, coarse_counts, coarse_inv):
        index = lax.axis_index("sx") * SIDE + lax.axis_index("sy")
        own = jnp.concatenate([coarse_basis[0].T[:KMAX - 1], kappa.reshape(1, M * M)], axis=0)
        mine = jnp.arange(LANES) // KMAX == index
        cnt = jnp.broadcast_to(jnp.where(mine, coarse_counts.astype(F32), 0.0)[None, :], (SUB, LANES))
        return pl.pallas_call(
            solve_kernel,
            out_shape=(jax.ShapeDtypeStruct((M, M, 2 * LANES), F32), jax.ShapeDtypeStruct((ITERS, 2 * LANES), F32)),
            in_specs=[any_spec] * 2 + [vmem_spec] * len(PIECES),
            out_specs=(any_spec, vmem_spec),
            scratch_shapes=scratch,
            compiler_params=pltpu.CompilerParams(collective_id=0, has_side_effects=True, vmem_limit_bytes=67043328),
        )(forcing, local_inv[0], own, coarse_inv, cnt)

    cell_spec = P(("batch", "sx"), "sy", None)
    sub_spec = P(("batch", "sx", "sy"), None, None)
    return jax.shard_map(body, mesh=mesh, in_specs=(cell_spec, P(("batch", "sx"), "sy"), sub_spec, sub_spec, P(("batch", "sx", "sy")), P("batch", None)), out_specs=(cell_spec, P("batch", None)), check_vma=False)
```

```python
import jax
import jax.numpy as jnp
from jax import lax
from jax.experimental import pallas as pl
from jax.experimental.pallas import tpu as pltpu
from jax.sharding import PartitionSpec as P

ITERS = 8
M = 32
D = 4
ME = M + 2 * D
NE = ME * ME
SUB = 8
LANES = 128
TILE = 256
KT = NE // TILE
KM = KT * TILE
REM = NE - KM
ROWS = 10
CHUNK = ROWS * ME
NP = NE + REM
NA = 208
BT = 16
NL = NE + 2 * BT
KMAX = 8
GRID = 128
LOW = M + SUB + D
WIDE = M + 2 * SUB
OWN = D + 1
STRIP = 9
EDGE = STRIP + 2
MESH = pl.DeviceIdType.MESH
HI = lax.Precision.HIGHEST
F32 = jnp.float32
BF16 = jnp.bfloat16
HALVES = (0, 1)
PIECES = (0, 1, 2)
FAR = (1, 2, 3)
LAST = FAR[-1]
SIDE = FAR[-1] + 1


def lanes(h):
    return slice(LANES * h, LANES * (h + 1))


def tile(k):
    return slice(TILE * k, TILE * (k + 1))


def mult(v, n=BT):
    return v if isinstance(v, int) else pl.multiple_of(v, n)


def row(v, k):
    return v[k:k + 1]


def wide(v):
    return jnp.broadcast_to(v, (SUB, LANES))


def colsum(v):
    return jnp.sum(v, axis=0, keepdims=True)


def each(copies, what):
    for c in copies:
        getattr(c, what)()


def split3(v):
    hi = v.astype(BF16)
    rest = v - hi.astype(F32)
    mid = rest.astype(BF16)
    low = (rest - mid.astype(F32)).astype(BF16)
    return hi, mid, low


def solve_kernel(f_hbm, inv_hbm, own_ref, cinv_ref, cnt_ref, x_hbm, nrm_ref,
                 S48, L, Lr, stage, X, Xr, T, TE, z, p, r, l, x, Q, Ey, W5, Ecat, RE, KB, FL,
               V, HB, HE, HP, PK, G1a, G2a, Gb, Gd, Ccat, cr, wr, cst, pqs,
               ld_sem, own_sem, h0_s, h0_r, v0_s, v0_r, h1_s, h1_r, v1_s, v1_r, v_s, v_r, hm_s, hm_r,
               a1_s, a1_r, a2_s, a2_r, b_s, b_r, d_s, d_r, out_sem):
    sx = lax.axis_index("sx")
    sy = lax.axis_index("sy")
    left, right = {"sy": sy - 1}, {"sy": sy + 1}
    has_left, has_right = sy > 0, sy < LAST
    has = (sx > 0, sx < LAST)
    near = lax.rem(sx, 2)
    inner = (sx > 0) & (sx < LAST)

    def rc(src, dst, s, q, dev):
        return pltpu.make_async_remote_copy(src, dst, s, q, device_id=dev, device_id_type=MESH)

    own = pl.ds(OWN, M)
    inv_cp = [pltpu.make_async_copy(inv_hbm.at[pl.ds(CHUNK * c, CHUNK)], stage.at[c], ld_sem.at[c]) for c in range(SIDE)]
    own_cp = [pltpu.make_async_copy(f_hbm.at[:, :, pl.ds(LANES * h, LANES)], S48.at[h, own, pl.ds(SUB, M)], own_sem.at[h]) for h in HALVES]
    each(own_cp, "start")
    each(inv_cp, "start")
    zrow = jnp.zeros((len(PIECES), OWN, WIDE, LANES), F32)
    S48[:, 0:OWN] = zrow
    S48[:, OWN + M:] = zrow
    zcol = jnp.zeros((len(PIECES), M, SUB, LANES), F32)
    S48[:, OWN:OWN + M, 0:SUB] = zcol
    S48[:, OWN:OWN + M, ME:] = zcol
    for b in (V, HB, HE, HP):
        b[...] = jnp.zeros(b.shape, F32)

    bar = pltpu.get_barrier_semaphore()
    peers = [{"sx": lax.rem(sx + k // SIDE, SIDE), "sy": lax.rem(sy + k % SIDE, SIDE)} for k in range(1, SIDE * SIDE)]
    for peer in peers:
        pl.semaphore_signal(bar, inc=1, device_id=peer, device_id_type=MESH)
    pl.semaphore_wait(bar, len(peers))

    def first_copies(G1, s, q):
        return [rc(G1.at[sy], G1.at[sy], s.at[d - 1], q.at[d - 1], {"sy": lax.rem(sy + d, SIDE)}) for d in FAR]

    a1 = first_copies(G1a, a1_s, a1_r)
    mine_y, mine_x = pl.ds(sy, 1), pl.ds(sx, 1)

    def gather(G, s, q):
        me = SIDE * sx + sy
        return me, [rc(G.at[me], G.at[me], s.at[k], q.at[k], peer) for k, peer in enumerate(peers)]
    sub4 = lax.broadcasted_iota(jnp.int32, (SIDE, LANES), 0)

    def send_rows(G, s, q, rows):
        me, copies = gather(G, s, q)
        v = jnp.zeros((SIDE, LANES), F32)
        for k, one in enumerate(rows):
            v = jnp.where(sub4 == k, one, v)
        G[pl.ds(me, 1)] = v[None]
        each(copies, "start")

    def full_sum(G, s, q):
        each(gather(G, s, q)[1], "wait")
        return jnp.sum(G[...], axis=0)

    send_rows(Gb, b_s, b_r, [row(cnt_ref[...], 0)])

    def halos(slabs, hs, hr, vs, vr):
        h = [rc(S48.at[slabs, own, pl.ds(SUB, SUB)], S48.at[slabs, own, pl.ds(ME, SUB)], hs.at[0], hr.at[0], left),
             rc(S48.at[slabs, own, pl.ds(M, SUB)], S48.at[slabs, own, pl.ds(0, SUB)], hs.at[1], hr.at[1], right)]
        v = [rc(S48.at[slabs, pl.ds(OWN, OWN)], S48.at[slabs, pl.ds(OWN + M, OWN)], vs.at[0], vr.at[1], {"sx": sx - 1}),
             rc(S48.at[slabs, pl.ds(M, OWN)], S48.at[slabs, pl.ds(0, OWN)], vs.at[1], vr.at[0], {"sx": sx + 1})]
        v_in = [rc(S48.at[slabs, pl.ds(0, OWN)], S48.at[slabs, pl.ds(0, OWN)], vs.at[e], vr.at[e], left) for e in HALVES]
        return h, v, v_in
    f_h, f_v, f_in = halos(pl.ds(0, 2), h0_s, h0_r, v0_s, v0_r)
    k_h, k_v, k_in = halos(pl.ds(2, 1), h1_s, h1_r, v1_s, v1_r)

    def go(pair):
        pl.when(has_left)(pair[0].start)
        pl.when(has_right)(pair[1].start)

    def come(pair):
        pl.when(has_right)(pair[0].wait_recv)
        pl.when(has_left)(pair[1].wait_recv)

    def gone(pair):
        pl.when(has_left)(pair[0].wait_send)
        pl.when(has_right)(pair[1].wait_send)

    def up_down(pair, what):
        for e in HALVES:
            pl.when(has[e])(getattr(pair[e], what))
    each(own_cp, "wait")
    go(f_h)

    slot = mult(KMAX * (sx * SIDE + sy), KMAX)
    FL[...] = jnp.zeros(FL.shape, F32)
    FL[pl.ds(slot, KMAX), 0:M * M] = own_ref[...]
    for k in range(SUB):
        S48[2, OWN + D * k:OWN + D * (k + 1), SUB:ME] = FL[:, lanes(k)].T.reshape(D, M, LANES)
    go(k_h)

    def shifted(v, k=D):
        return pltpu.roll(v, WIDE - k, 0)[0:ME]
    lane_of = lax.broadcasted_iota(jnp.int32, (WIDE, LANES), 1)
    last_slot = lane_of % KMAX == KMAX - 1

    def basis_of(v):
        return jnp.where(last_slot[0:ME], 0.0, v)

    def own_rows(i, c):
        mine = S48[2, i + 1, SUB:ME]
        mine = jnp.concatenate([mine, jnp.zeros((BT, LANES), F32)], axis=0)
        W5[0, i] = basis_of(pltpu.roll(mine, D, 0)[0:ME])
        return c
    for i in list(range(D)) + list(range(D + M, ME)):
        W5[0, i] = jnp.zeros((ME, LANES), F32)
    lax.fori_loop(D, D + M, own_rows, 0)
    flat = W5[0].reshape(NE, LANES)
    for k in range(NP // LANES):
        blk = flat[LANES * k:LANES * (k + 1)]
        if blk.shape[0] < LANES:
            blk = jnp.concatenate([blk, jnp.zeros_like(blk)], axis=0)
        FL[:, lanes(k)] = blk.T
    restrict = FL[pl.ds(slot, KMAX), 0:NE]
    restrict = jnp.concatenate([restrict, jnp.zeros_like(restrict)], axis=0)

    for b in (p, z, r, l, x, T):
        def zero(i, c, b=b):
            b[:, pl.ds(i, 1)] = jnp.zeros((2, 1, ME, LANES), F32)
            return c
        lax.fori_loop(0, b.shape[1], zero, 0)
    Xr[...] = jnp.zeros(Xr.shape, BF16)
    for b in (cr, wr, cst, pqs, nrm_ref):
        b[...] = jnp.zeros(b.shape, F32)

    def put_l(v, rows):
        one, two, three = split3(v)
        rest = []
        for k, piece in enumerate((one, two, three)):
            L[rows, KM * k:KM * (k + 1)] = piece[:, 0:KM]
            rest.append(piece[:, KM:].astype(F32))
        twice = jnp.concatenate(rest[0:2], axis=1).astype(BF16)
        Lr[rows, lanes(0)] = twice
        Lr[rows, lanes(1)] = twice
        Lr[rows, lanes(2)] = jnp.concatenate([rest[0], rest[2]], axis=1).astype(BF16)
        Lr[rows, lanes(LAST)] = jnp.zeros(twice.shape, BF16)

    for at in (0, LAST * CHUNK + BT):
        put_l(restrict, pl.ds(at, BT))

    def split_inv(c):
        inv_cp[c].wait()

        def body(k, carry):
            put_l(stage[c, pl.ds(mult(BT * k), BT), :], pl.ds(mult(CHUNK * c + BT * (c // LAST + 1) + BT * k), BT))
            return carry
        lax.fori_loop(0, CHUNK // BT, body, 0)

    split_inv(0)
    split_inv(1)
    come(f_h)
    gone(f_h)
    up_down(f_v, "start")
    split_inv(2)
    split_inv(LAST)

    def dot(a, b):
        return jnp.dot(a, b, preferred_element_type=F32)

    def dot_pieces(lhs, v):
        y1, y2, y3 = split3(v)
        total = 0.0
        for n, two in enumerate(((y1, y1), (y2, y2), (y3, y1))):
            total = total + dot(lhs(LANES * (n // 2)), jnp.concatenate(two, axis=0))
        return total

    cnt = wide(row(full_sum(Gb, b_s, b_r), 0))
    lane = lax.broadcasted_iota(jnp.int32, (SUB, LANES), 1)
    starts = cnt
    for d in (KMAX, 2 * KMAX, D * KMAX, SUB * KMAX):
        starts = starts + jnp.where(lane >= d, pltpu.roll(starts, d, 1), 0.0)
    starts = starts - cnt
    col = (lane % KMAX).astype(F32)
    target = jnp.where(col < cnt, starts + col, -1.0)
    half = cinv_ref.shape[0]
    pick = jnp.where(lax.broadcasted_iota(jnp.int32, (half, LANES), 0).astype(F32) == row(target, 0), 1.0, 0.0)

    def rhs_of(parts):
        v = jnp.concatenate(parts + [jnp.zeros_like(parts[0])], axis=0)
        return v.astype(BF16)

    def lhs_of(parts):
        v = jnp.concatenate(parts + [jnp.zeros_like(parts[0])], axis=1)
        return v.astype(BF16)

    def as_f32(v):
        return [piece.astype(F32) for piece in split3(v)]
    spread = dot(lhs_of(as_f32(cinv_ref[...])), rhs_of([pick] * len(PIECES)))
    spread = dot(lhs_of([pick.T] * len(PIECES)), rhs_of(as_f32(spread)))

    def put_middle(ref, rows, v):
        for k, piece in zip((1, 0, 2), split3(v)):
            ref[rows, lanes(k)] = piece
    put_middle(Ccat, pl.ds(0, LANES), spread)

    come(k_h)
    gone(k_h)
    up_down(k_v, "start")
    up_down(f_v, "wait_send")
    up_down(f_in, "wait_recv")

    jcol = lax.broadcasted_iota(jnp.int32, (ME, LANES), 0)
    gj = sy * M + jcol - D
    in_col = (gj >= 0) & (gj < GRID)

    def kappa_rows(i, c):
        KB[i] = jnp.broadcast_to(jnp.sum(jnp.where(last_slot, S48[2, i], 0.0), axis=1, keepdims=True), (WIDE, LANES))
        return c

    def weights(i, c):
        gi = sx * M + i - D
        ok = in_col & (gi >= 0) & (gi < GRID)
        here = KB[i + 1]
        kc = shifted(here)

        def pair(other, inside):
            both = ok & inside
            w = jnp.where(both, 2.0 * kc * other / jnp.where(both, kc + other, 1.0), 0.0)
            return w, jnp.where(ok & jnp.logical_not(inside), kc, w)
        edges = (pair(shifted(KB[i]), ok & (gi > 0)), pair(shifted(KB[i + 2]), ok & (gi < GRID - 1)),
                 pair(shifted(here, D - 1), gj > 0), pair(shifted(here, D + 1), gj < GRID - 1))
        total = 0.0
        for k, (w, d) in enumerate(edges):
            W5[k, i] = w
            total = total + d
        W5[SIDE, i] = total
        return c

    def pair_of(two, k):
        return jnp.concatenate(two, axis=0), pl.ds(mult(2 * ME * k), 2 * ME)

    def basis_rows(k, c):
        v, rows = pair_of([basis_of(shifted(S48[2, 2 * k + j])) for j in HALVES], k)
        put_middle(Ecat, rows, v)
        return c
    def geometry():
        up_down(k_v, "wait_send")
        up_down(k_in, "wait_recv")
        lax.fori_loop(0, M + 2 * OWN, kappa_rows, 0)
        lax.fori_loop(0, ME, weights, 0)
        for i in range(ME):
            RE[0, i:i + 1] = S48[2, i + 1, D - 1:D]
            RE[1, i:i + 1] = S48[2, i + 1, LOW:LOW + 1]
        lax.fori_loop(0, LOW // 2 - 1, basis_rows, 0)
        v, rows = pair_of([basis_of(RE[j]) for j in HALVES], LOW // 2 - 1)
        put_middle(Ecat, rows, v)

    def put_x(two, h, k):
        v, rows = pair_of(two, k)
        for j, piece in enumerate(split3(v)):
            X[j, rows, lanes(h)] = piece

    def put_rest():
        for slot, j in enumerate((0, 0, 1, 1, 2, 0)):
            Xr[REM * slot:REM * (slot + 1), :] = X[j, KM:NE, :]

    def first_rows(k, c):
        for h in HALVES:
            two = [shifted(S48[h, 2 * k + 1 + j]) for j in HALVES]
            for j in HALVES:
                Q[h, 2 * k + 1 + j] = two[j]
            put_x(two, h, k)
        return c
    lax.fori_loop(0, ME // 2, first_rows, 0)
    put_rest()

    colf = jnp.where((jcol >= D) & (jcol < D + M), 1.0, 0.0)
    sub8 = lax.broadcasted_iota(jnp.int32, (SUB, LANES), 0)
    zero = jnp.zeros((ME, LANES), F32)

    def product(start, n):
        first = NA
        outs = []
        for at, size in ((0, first), (first, n - first)):
            rows = pl.ds(mult(start + at), size)
            total = dot(Lr[rows, :], Xr[...])
            for j in PIECES:
                for i in PIECES[:len(PIECES) - j]:
                    total = total + dot(L[rows, KM * i:KM * (i + 1)], X[j, 0:KM, :])
            outs.append(total)
        return outs

    def put_t(outs, c):
        at = 0
        for v in outs:
            while v.shape[0]:
                top, off = 1 + ROWS * c + at // ME, at % ME
                n = min(ME - off, v.shape[0]) if off or v.shape[0] < ME else v.shape[0] // ME * ME
                whole = max(n // ME, 1)
                for h in HALVES:
                    T[h, pl.ds(top, whole), off:off + n // whole] = v[0:n, lanes(h)].reshape(whole, n // whole, LANES)
                v, at = v[n:], at + n

    def v_copy(e, par):
        return rc(T.at[:, pl.ds(1 + (M - 1) * e, STRIP)], V.at[par, 1 - e], v_s.at[e], v_r.at[par, 1 - e], {"sx": sx - 1 + 2 * e})

    def v_wait(e, par):
        v_copy(e, par).wait_send()
        rc(T.at[:, pl.ds(1, STRIP)], V.at[par, e], v_s.at[e], v_r.at[par, e], left).wait_recv()

    def step(m, carry):
        par = lax.rem(m, 2)

        def side(n, src, dst):
            return [rc(src[j], dst.at[par, 1 - j], hm_s.at[par, j, n], hm_r.at[par, 1 - j, n], (left, right)[j]) for j in HALVES]

        def cols(ref, lo, n):
            return [ref.at[:, pl.ds(lo, n), pl.ds(M * j, SUB)] for j in HALVES]

        mids = [side(n, cols(T, EDGE + ROWS * n, ROWS), HB.at[:, :, n]) for n in HALVES]
        edges = [side(2 + e, cols(TE, EDGE * e, EDGE), HE.at[:, :, e]) for e in (near, 1 - near)]
        parts = ((mult(BT * (1 - near)), ME - BT), (mult((ME - BT) * near, SUB), BT))
        rings = [side(SIDE + n, [PK.at[j, :, pl.ds(at, size)] for j in HALVES], HP.at[:, :, :, pl.ds(at, size)])
                 for n, (at, size) in enumerate(parts)]
        everything = mids + edges + rings
        v_near, v_far = v_copy(near, par), v_copy(1 - near, par)
        a2 = [rc(G1a, G2a.at[par, sx], a2_s.at[d - 1], a2_r.at[par, d - 1], {"sx": lax.rem(sx + d, SIDE)}) for d in FAR]

        def edge(e, pair):
            for h in HALVES:
                TE[h, pl.ds((EDGE + 2) * e, STRIP)] = T[h, pl.ds((M + 1) * e, STRIP)] + V[par, e, h]
                TE[h, pl.ds(STRIP + 2 * e, 2)] = T[h, pl.ds(STRIP + 2 * EDGE * e, 2)]
            go(pair)

        def ring_rows(pairs):
            for h in HALVES:
                for at, ref, k in pairs:
                    for j, lane in enumerate((SUB, M - 1)):
                        PK[j, h, at] = ref[h, k, lane:lane + 1]

        def ring_edge(e):
            for h in HALVES:
                for k in range(ROWS):
                    for j, lane in enumerate((SUB, M - 1)):
                        PK[j, h, pl.ds((M - 2) * e + k, 1)] = TE[h, pl.ds(ROWS * e + 1 + k, 1), lane:lane + 1].reshape(1, LANES)

        first = m == 0
        c_near, c_far = LAST * near, LAST * (1 - near)
        start = (LAST * CHUNK + BT) * near
        send_rows(Gd, d_s, d_r, [row(pqs[h], 0) for h in HALVES])
        out = product((LAST * CHUNK + BT) - start, CHUNK + BT)
        put_t([out[0][BT:], out[1]], c_far)
        for h in HALVES:
            G1a[mine_y, h] = out[0][0:SUB, lanes(h)][None]
        each(a1, "start")
        v_far.start()
        put_t(product(BT + start, CHUNK), c_near)
        pl.when(inner)(v_near.start)
        pl.when(jnp.logical_not(inner))(lambda: edge(near, edges[0]))
        v_wait(1 - near, par)
        edge(1 - near, edges[1])
        put_t(product(BT + CHUNK, CHUNK), 1)
        go(mids[0])
        each(a1, "wait")
        each(a2, "start")

        pq = full_sum(Gd, d_s, d_r)
        alpha = [jnp.where(first, -1.0, row(cst[0, h], 0) / row(pq, h)) for h in HALVES]

        tot = [[zero, zero] for h in HALVES]

        def update(c, inside):
            for h in HALVES:
                for k in range(ROWS):
                    i = 1 + ROWS * c + k
                    rn = r[h, i] - alpha[h] * Q[h, i]
                    ln = l[h, i] - alpha[h] * T[h, i]
                    r[h, i] = rn
                    l[h, i] = ln
                    x[h, i] = x[h, i] + alpha[h] * p[h, i]
                    w = colf if inside else jnp.where((i >= OWN) & (i < OWN + M), 1.0, 0.0) * colf
                    tot[h][0] = tot[h][0] + rn * ln
                    tot[h][1] = tot[h][1] + w * (rn * rn)

        out = product(BT + 2 * CHUNK, CHUNK)
        update(c_far, False)
        update(c_near, False)
        update(1, True)
        put_t(out, 2)
        update(2, True)
        G2a[par, mine_x] = G1a[...][None]
        each(a2, "wait_send")
        send_rows(Gb, b_s, b_r, [colsum(v) for two in tot for v in two])
        go(mids[1])
        ring_rows([(slice(i - 1, i), T, i) for i in range(EDGE, M - 1)])
        ring_edge(1 - near)
        go(rings[0])

        @pl.when(inner)
        def _():
            v_wait(near, par)
            edge(near, edges[0])
        ring_edge(near)
        go(rings[1])

        pl.when(first)(geometry)
        each(a2, "wait_recv")
        cq = jnp.concatenate([G2a[par, :, :, h].reshape(LANES, LANES) for h in HALVES], axis=1)
        yq = dot_pieces(lambda at: Ccat[:, at:at + TILE], cq)
        rzc = []
        for h in HALVES:
            cr[h] = cr[h] - alpha[h] * cq[:, lanes(h)]
            wr[h] = wr[h] - alpha[h] * yq[:, lanes(h)]
            rzc.append(colsum(cr[h] * wr[h]))
        n = LOW // 2
        for part in HALVES:
            o = dot_pieces(lambda at: Ecat[ME * n * part:ME * n * (part + 1), at:at + TILE], yq)
            for h in HALVES:
                Ey[h, n * part:n * (part + 1)] = o[:, lanes(h)].reshape(n, ME, LANES)

        got = full_sum(Gb, b_s, b_r)
        beta = []
        for h in HALVES:
            rzn = row(got, 2 * h) + rzc[h]
            rr = row(got, 2 * h + 1)
            beta.append(jnp.where(first, 0.0, rzn / row(cst[0, h], 0)))
            ff = jnp.where(first, jnp.sqrt(rr), row(cst[1, h], 0))
            cst[0, h] = wide(rzn)
            cst[1, h] = wide(ff)
            nrm_ref[:, lanes(h)] = jnp.where(sub8 == m - 1, jnp.sqrt(rr) / ff, nrm_ref[:, lanes(h)])

        def renew(i, u):
            for h in HALVES:
                zn = z[h, i] - alpha[h] * (u[h] + Ey[h, i])
                z[h, i] = zn
                p[h, i] = zn + beta[h] * p[h, i]

        def sides(b, buf, n, h, k):
            return jnp.concatenate([b[0:SUB] + buf[par, 0, n, h, k], b[SUB:M], b[M:] + buf[par, 1, n, h, k]], axis=0)

        def mid_rows(n):
            def body(k, c):
                i = EDGE + ROWS * n + k
                renew(i, [sides(T[h, i], HB, n, h, k) for h in HALVES])
                return c
            come(mids[n])
            lax.fori_loop(0, ROWS, body, 0)

        def edge_rows(e, pair):
            def body(k, c):
                renew((M - 1) * e + k, [sides(TE[h, EDGE * e + k], HE, e, h, k) for h in HALVES])
                return c
            come(pair)
            lax.fori_loop(0, EDGE, body, 0)

        def ring_cells(n):
            come(rings[n])
            at = pl.ds(*parts[n])
            for h in HALVES:
                for j in HALVES:
                    i = LOW - 2 + j
                    zn = z[h, i, at] - alpha[h] * (HP[par, j, h, at] + Ey[h, i, at])
                    z[h, i, at] = zn
                    p[h, i, at] = zn + beta[h] * p[h, i, at]

        def apply_rows(g, car):
            sums = list(car)
            rings = [[p[h, LOW - 2 + j, pl.ds(mult(SUB * g, SUB), SUB), :] for j in HALVES] for h in HALVES]
            rows = [[], []]
            for k in range(SUB):
                i = SUB * g + k
                w = [W5[j, i] for j in range(SIDE + 1)]
                own_f = jnp.where((i >= D) & (i < D + M), 1.0, 0.0) * colf
                for h in HALVES:
                    c = p[h, i + 1]
                    west = jnp.where(jcol == 0, row(rings[h][0], k), pltpu.roll(c, 1, 0))
                    east = jnp.where(jcol == ME - 1, row(rings[h][1], k), pltpu.roll(c, ME - 1, 0))
                    q = w[SIDE] * c
                    for j, other in enumerate((p[h, i], p[h, i + 2], west, east)):
                        q = q - w[j] * other
                    Q[h, i + 1] = q
                    sums[h] = sums[h] + own_f * (c * q)
                    rows[h].append(q)
                    if len(rows[h]) == 2:
                        put_x(rows[h], h, D * g + k // 2)
                        rows[h] = []
            return tuple(sums)
        edge_rows(1 - near, edges[1])
        mid_rows(0)
        mid_rows(1)
        ring_cells(0)
        low = 2 * (1 - near)
        car = lax.fori_loop(low, low + LAST, apply_rows, (zero, zero))
        edge_rows(near, edges[0])
        ring_cells(1)
        low = LAST * near
        car = lax.fori_loop(low, low + 2, apply_rows, car)
        put_rest()
        for h in HALVES:
            pqs[h] = wide(colsum(car[h]))

        for pair in everything:
            gone(pair)
        return carry

    lax.fori_loop(0, ITERS, step, 0)

    send_rows(Gd, d_s, d_r, [row(pqs[h], 0) for h in HALVES])
    pq = full_sum(Gd, d_s, d_r)
    alpha = [row(cst[0, h], 0) / row(pq, h) for h in HALVES]

    def finish(i, car):
        res = []
        for h in HALVES:
            rn = r[h, i] - alpha[h] * Q[h, i]
            res.append(car[h] + colf * (rn * rn))
            xn = x[h, i] + alpha[h] * p[h, i]
            T[h, i, 0:M] = pltpu.roll(jnp.concatenate([xn, xn[0:SUB]], axis=0), WIDE - D, 0)[0:M]
        return tuple(res)
    rr = lax.fori_loop(OWN, OWN + M, finish, (zero, zero))
    out_cp = [pltpu.make_async_copy(T.at[h, own, pl.ds(0, M)], x_hbm.at[:, :, pl.ds(LANES * h, LANES)], out_sem.at[h]) for h in HALVES]
    each(out_cp, "start")
    send_rows(Gb, b_s, b_r, [colsum(v) for v in rr])
    got = full_sum(Gb, b_s, b_r)
    for h in HALVES:
        nrm_ref[:, lanes(h)] = jnp.where(sub8 == ITERS - 1, jnp.sqrt(row(got, h)) / row(cst[1, h], 0), nrm_ref[:, lanes(h)])
    each(out_cp, "wait")


def solution(mesh):
    def dma(*shape):
        return pltpu.SemaphoreType.DMA(shape)

    def vm(*shape, dtype=F32):
        return pltpu.VMEM(shape, dtype)

    field = vm(2, LOW, ME, LANES)
    strips = [vm(2, 2, 2, 2, n, SUB, LANES) for n in (ROWS, EDGE)]
    gathers = [vm(SIDE, 2, SUB, LANES), vm(2, SIDE, SIDE, 2, SUB, LANES)] + [vm(SIDE * SIDE, SIDE, LANES)] * 2
    scratch = [
        vm(len(PIECES), M + 2 * OWN, WIDE, LANES), vm(NL, KM * len(PIECES), dtype=BF16), vm(NL, 2 * TILE, dtype=BF16),
        vm(SIDE, CHUNK, NE), vm(len(PIECES), NE, TILE, dtype=BF16), vm(2 * TILE, TILE, dtype=BF16),
        field, vm(2, 2 * EDGE, ME, LANES), field, field, field, field, field, field, field,
        vm(SIDE + 1, ME, ME, LANES), vm(LOW * ME, LANES * len(PIECES), dtype=BF16), vm(2, ME, LANES), vm(M + 2 * OWN, WIDE, LANES), vm(LANES, NP),
        vm(2, 2, 2, STRIP, ME, LANES), *strips, vm(2, 2, 2, ME, LANES), vm(2, 2, ME, LANES), *gathers,
        vm(LANES, LANES * len(PIECES), dtype=BF16), vm(2, LANES, LANES), vm(2, LANES, LANES), vm(2, 2, SUB, LANES),
        vm(2, SUB, LANES), dma(SIDE), dma(2), *[dma(2)] * 9, dma(2, 2), *[dma(2, 2, SIDE + 2)] * 2,
        *[dma(LAST)] * 3, dma(2, LAST), *[dma(SIDE * SIDE - 1)] * 4, dma(2),
    ]
    any_spec = pl.BlockSpec(memory_space=pl.ANY)
    vmem_spec = pl.BlockSpec(memory_space=pltpu.VMEM)

    def body(forcing, kappa, local_inv, coarse_basis, coarse_counts, coarse_inv):
        index = lax.axis_index("sx") * SIDE + lax.axis_index("sy")
        own = jnp.concatenate([coarse_basis[0].T[:KMAX - 1], kappa.reshape(1, M * M)], axis=0)
        mine = jnp.arange(LANES) // KMAX == index
        cnt = jnp.broadcast_to(jnp.where(mine, coarse_counts.astype(F32), 0.0)[None, :], (SUB, LANES))
        return pl.pallas_call(
            solve_kernel,
            out_shape=(jax.ShapeDtypeStruct((M, M, 2 * LANES), F32), jax.ShapeDtypeStruct((ITERS, 2 * LANES), F32)),
            in_specs=[any_spec] * 2 + [vmem_spec] * len(PIECES),
            out_specs=(any_spec, vmem_spec),
            scratch_shapes=scratch,
            compiler_params=pltpu.CompilerParams(collective_id=0, has_side_effects=True, vmem_limit_bytes=67043328),
        )(forcing, local_inv[0], own, coarse_inv, cnt)

    cell_spec = P(("batch", "sx"), "sy", None)
    sub_spec = P(("batch", "sx", "sy"), None, None)
    return jax.shard_map(body, mesh=mesh, in_specs=(cell_spec, P(("batch", "sx"), "sy"), sub_spec, sub_spec, P(("batch", "sx", "sy")), P("batch", None)), out_specs=(cell_spec, P("batch", None)), check_vma=False)
```

```python
import jax
import jax.numpy as jnp
from jax import lax
from jax.experimental import pallas as pl
from jax.experimental.pallas import tpu as pltpu
from jax.sharding import PartitionSpec as P

ITERS = 8
M = 32
D = 4
ME = M + 2 * D
NE = ME * ME
SUB = 8
LANES = 128
TILE = 256
KT = NE // TILE
KM = KT * TILE
REM = NE - KM
ROWS = 10
CHUNK = ROWS * ME
NP = NE + REM
NA = 208
BT = 16
NL = NE + 2 * BT
KMAX = 8
GRID = 128
LOW = M + SUB + D
WIDE = M + 2 * SUB
OWN = D + 1
STRIP = 9
EDGE = STRIP + 2
MESH = pl.DeviceIdType.MESH
HI = lax.Precision.HIGHEST
F32 = jnp.float32
BF16 = jnp.bfloat16
HALVES = (0, 1)
PIECES = (0, 1, 2)
FAR = (1, 2, 3)
LAST = FAR[-1]
SIDE = FAR[-1] + 1


def lanes(h):
    return slice(LANES * h, LANES * (h + 1))


def tile(k):
    return slice(TILE * k, TILE * (k + 1))


def mult(v, n=BT):
    return v if isinstance(v, int) else pl.multiple_of(v, n)


def row(v, k):
    return v[k:k + 1]


def wide(v):
    return jnp.broadcast_to(v, (SUB, LANES))


def colsum(v):
    return jnp.sum(v, axis=0, keepdims=True)


def each(copies, what):
    for c in copies:
        getattr(c, what)()


def split3(v):
    hi = v.astype(BF16)
    rest = v - hi.astype(F32)
    mid = rest.astype(BF16)
    low = (rest - mid.astype(F32)).astype(BF16)
    return hi, mid, low


def solve_kernel(f_hbm, inv_hbm, own_ref, cinv_ref, cnt_ref, x_hbm, nrm_ref,
                 S48, L, Lr, stage, X, Xr, T, TE, z, p, r, l, x, Q, Ey, W5, Ecat, RE, KB, FL, PF, RF,
               V, HB, HE, HP, PK, G1a, G2a, Gb, Gd, Ccat, cr, wr, cst, pqs,
               ld_sem, own_sem, h0_s, h0_r, v0_s, v0_r, h1_s, h1_r, v1_s, v1_r, v_s, v_r, hm_s, hm_r,
               a1_s, a1_r, a2_s, a2_r, b_s, b_r, d_s, d_r, out_sem):
    sx = lax.axis_index("sx")
    sy = lax.axis_index("sy")
    left, right = {"sy": sy - 1}, {"sy": sy + 1}
    has_left, has_right = sy > 0, sy < LAST
    has = (sx > 0, sx < LAST)
    near = lax.rem(sx, 2)
    inner = (sx > 0) & (sx < LAST)

    def rc(src, dst, s, q, dev):
        return pltpu.make_async_remote_copy(src, dst, s, q, device_id=dev, device_id_type=MESH)

    own = pl.ds(OWN, M)
    inv_cp = [pltpu.make_async_copy(inv_hbm.at[pl.ds(CHUNK * c, CHUNK)], stage.at[c], ld_sem.at[c]) for c in range(SIDE)]
    own_cp = [pltpu.make_async_copy(f_hbm.at[:, :, pl.ds(LANES * h, LANES)], S48.at[h, own, pl.ds(SUB, M)], own_sem.at[h]) for h in HALVES]
    each(own_cp, "start")
    each(inv_cp, "start")
    zrow = jnp.zeros((len(PIECES), OWN, WIDE, LANES), F32)
    S48[:, 0:OWN] = zrow
    S48[:, OWN + M:] = zrow
    zcol = jnp.zeros((len(PIECES), M, SUB, LANES), F32)
    S48[:, OWN:OWN + M, 0:SUB] = zcol
    S48[:, OWN:OWN + M, ME:] = zcol
    for b in (V, HB, HE, HP, RF):
        b[...] = jnp.zeros(b.shape, F32)

    bar = pltpu.get_barrier_semaphore()
    peers = [{"sx": lax.rem(sx + k // SIDE, SIDE), "sy": lax.rem(sy + k % SIDE, SIDE)} for k in range(1, SIDE * SIDE)]
    for peer in peers:
        pl.semaphore_signal(bar, inc=1, device_id=peer, device_id_type=MESH)
    pl.semaphore_wait(bar, len(peers))

    def first_copies(G1, s, q):
        return [rc(G1.at[sy], G1.at[sy], s.at[d - 1], q.at[d - 1], {"sy": lax.rem(sy + d, SIDE)}) for d in FAR]

    a1 = first_copies(G1a, a1_s, a1_r)
    mine_y, mine_x = pl.ds(sy, 1), pl.ds(sx, 1)

    def gather(G, s, q):
        me = SIDE * sx + sy
        return me, [rc(G.at[me], G.at[me], s.at[k], q.at[k], peer) for k, peer in enumerate(peers)]
    sub4 = lax.broadcasted_iota(jnp.int32, (SIDE, LANES), 0)

    def send_rows(G, s, q, rows):
        me, copies = gather(G, s, q)
        v = jnp.zeros((SIDE, LANES), F32)
        for k, one in enumerate(rows):
            v = jnp.where(sub4 == k, one, v)
        G[pl.ds(me, 1)] = v[None]
        each(copies, "start")

    def full_sum(G, s, q):
        each(gather(G, s, q)[1], "wait")
        return jnp.sum(G[...], axis=0)

    send_rows(Gb, b_s, b_r, [row(cnt_ref[...], 0)])

    def halos(slabs, hs, hr, vs, vr):
        h = [rc(S48.at[slabs, own, pl.ds(SUB, SUB)], S48.at[slabs, own, pl.ds(ME, SUB)], hs.at[0], hr.at[0], left),
             rc(S48.at[slabs, own, pl.ds(M, SUB)], S48.at[slabs, own, pl.ds(0, SUB)], hs.at[1], hr.at[1], right)]
        v = [rc(S48.at[slabs, pl.ds(OWN, OWN)], S48.at[slabs, pl.ds(OWN + M, OWN)], vs.at[0], vr.at[1], {"sx": sx - 1}),
             rc(S48.at[slabs, pl.ds(M, OWN)], S48.at[slabs, pl.ds(0, OWN)], vs.at[1], vr.at[0], {"sx": sx + 1})]
        v_in = [rc(S48.at[slabs, pl.ds(0, OWN)], S48.at[slabs, pl.ds(0, OWN)], vs.at[e], vr.at[e], left) for e in HALVES]
        return h, v, v_in
    _, f_v, f_in = halos(pl.ds(0, 2), h0_s, h0_r, v0_s, v0_r)
    f_h = [rc(PF.at[j], RF.at[1 - j], h0_s.at[j], h0_r.at[j], (left, right)[j]) for j in HALVES]
    k_h, k_v, k_in = halos(pl.ds(2, 1), h1_s, h1_r, v1_s, v1_r)

    def go(pair):
        pl.when(has_left)(pair[0].start)
        pl.when(has_right)(pair[1].start)

    def come(pair):
        pl.when(has_right)(pair[0].wait_recv)
        pl.when(has_left)(pair[1].wait_recv)

    def gone(pair):
        pl.when(has_left)(pair[0].wait_send)
        pl.when(has_right)(pair[1].wait_send)

    def up_down(pair, what):
        for e in HALVES:
            pl.when(has[e])(getattr(pair[e], what))
    each(own_cp, "wait")
    lower = lax.broadcasted_iota(jnp.int32, (SUB, LANES), 0) < D

    def pack(k, c):
        for h in HALVES:
            for j in HALVES:
                a, b = [S48[h, OWN + 2 * k + n, (M if j else SUB):(ME if j else 2 * SUB)] for n in HALVES]
                PF[j, h, k] = jnp.where(lower, pltpu.roll(a, D, 0), b) if j else jnp.where(lower, a, pltpu.roll(b, D, 0))
        return c

    def unpack(k, c):
        for h in HALVES:
            for j in HALVES:
                v = RF[j, h, k]
                two = (v, pltpu.roll(v, D, 0))
                for n in HALVES:
                    S48[h, OWN + 2 * k + n, (ME if j else 0):(WIDE if j else SUB)] = two[n if j else 1 - n]
        return c
    lax.fori_loop(0, M // 2, pack, 0)
    go(f_h)

    slot = mult(KMAX * (sx * SIDE + sy), KMAX)
    FL[...] = jnp.zeros(FL.shape, F32)
    FL[pl.ds(slot, KMAX), 0:M * M] = own_ref[...]
    for k in range(SUB):
        S48[2, OWN + D * k:OWN + D * (k + 1), SUB:ME] = FL[:, lanes(k)].T.reshape(D, M, LANES)
    go(k_h)

    def shifted(v, k=D):
        return pltpu.roll(v, WIDE - k, 0)[0:ME]
    lane_of = lax.broadcasted_iota(jnp.int32, (WIDE, LANES), 1)
    last_slot = lane_of % KMAX == KMAX - 1

    def basis_of(v):
        return jnp.where(last_slot[0:ME], 0.0, v)

    def own_rows(i, c):
        mine = S48[2, i + 1, SUB:ME]
        mine = jnp.concatenate([mine, jnp.zeros((BT, LANES), F32)], axis=0)
        W5[0, i] = basis_of(pltpu.roll(mine, D, 0)[0:ME])
        return c
    for i in list(range(D)) + list(range(D + M, ME)):
        W5[0, i] = jnp.zeros((ME, LANES), F32)
    lax.fori_loop(D, D + M, own_rows, 0)
    flat = W5[0].reshape(NE, LANES)
    for k in range(NP // LANES):
        blk = flat[LANES * k:LANES * (k + 1)]
        if blk.shape[0] < LANES:
            blk = jnp.concatenate([blk, jnp.zeros_like(blk)], axis=0)
        FL[:, lanes(k)] = blk.T
    restrict = FL[pl.ds(slot, KMAX), 0:NE]
    restrict = jnp.concatenate([restrict, jnp.zeros_like(restrict)], axis=0)

    for b in (p, z, r, l, x, T):
        def zero(i, c, b=b):
            b[:, pl.ds(i, 1)] = jnp.zeros((2, 1, ME, LANES), F32)
            return c
        lax.fori_loop(0, b.shape[1], zero, 0)
    Xr[...] = jnp.zeros(Xr.shape, BF16)
    for b in (cr, wr, cst, pqs, nrm_ref):
        b[...] = jnp.zeros(b.shape, F32)

    def put_l(v, rows):
        one, two, three = split3(v)
        rest = []
        for k, piece in enumerate((one, two, three)):
            L[rows, KM * k:KM * (k + 1)] = piece[:, 0:KM]
            rest.append(piece[:, KM:].astype(F32))
        twice = jnp.concatenate(rest[0:2], axis=1).astype(BF16)
        Lr[rows, lanes(0)] = twice
        Lr[rows, lanes(1)] = twice
        Lr[rows, lanes(2)] = jnp.concatenate([rest[0], rest[2]], axis=1).astype(BF16)
        Lr[rows, lanes(LAST)] = jnp.zeros(twice.shape, BF16)

    for at in (0, LAST * CHUNK + BT):
        put_l(restrict, pl.ds(at, BT))

    def split_inv(c):
        inv_cp[c].wait()

        def body(k, carry):
            put_l(stage[c, pl.ds(mult(BT * k), BT), :], pl.ds(mult(CHUNK * c + BT * (c // LAST + 1) + BT * k), BT))
            return carry
        lax.fori_loop(0, CHUNK // BT, body, 0)

    split_inv(0)
    split_inv(1)
    come(f_h)
    gone(f_h)
    lax.fori_loop(0, M // 2, unpack, 0)
    up_down(f_v, "start")
    split_inv(2)
    split_inv(LAST)

    def dot(a, b):
        return jnp.dot(a, b, preferred_element_type=F32)

    def dot_pieces(lhs, v):
        y1, y2, y3 = split3(v)
        total = 0.0
        for n, two in enumerate(((y1, y1), (y2, y2), (y3, y1))):
            total = total + dot(lhs(LANES * (n // 2)), jnp.concatenate(two, axis=0))
        return total

    cnt = wide(row(full_sum(Gb, b_s, b_r), 0))
    lane = lax.broadcasted_iota(jnp.int32, (SUB, LANES), 1)
    starts = cnt
    for d in (KMAX, 2 * KMAX, D * KMAX, SUB * KMAX):
        starts = starts + jnp.where(lane >= d, pltpu.roll(starts, d, 1), 0.0)
    starts = starts - cnt
    col = (lane % KMAX).astype(F32)
    target = jnp.where(col < cnt, starts + col, -1.0)
    half = cinv_ref.shape[0]
    pick = jnp.where(lax.broadcasted_iota(jnp.int32, (half, LANES), 0).astype(F32) == row(target, 0), 1.0, 0.0)

    def rhs_of(parts):
        v = jnp.concatenate(parts + [jnp.zeros_like(parts[0])], axis=0)
        return v.astype(BF16)

    def lhs_of(parts):
        v = jnp.concatenate(parts + [jnp.zeros_like(parts[0])], axis=1)
        return v.astype(BF16)

    def as_f32(v):
        return [piece.astype(F32) for piece in split3(v)]
    spread = dot(lhs_of(as_f32(cinv_ref[...])), rhs_of([pick] * len(PIECES)))
    spread = dot(lhs_of([pick.T] * len(PIECES)), rhs_of(as_f32(spread)))

    def put_middle(ref, rows, v):
        for k, piece in zip((1, 0, 2), split3(v)):
            ref[rows, lanes(k)] = piece
    put_middle(Ccat, pl.ds(0, LANES), spread)

    come(k_h)
    gone(k_h)
    up_down(k_v, "start")
    up_down(f_v, "wait_send")
    up_down(f_in, "wait_recv")

    jcol = lax.broadcasted_iota(jnp.int32, (ME, LANES), 0)
    gj = sy * M + jcol - D
    in_col = (gj >= 0) & (gj < GRID)

    def kappa_rows(i, c):
        KB[i] = jnp.broadcast_to(jnp.sum(jnp.where(last_slot, S48[2, i], 0.0), axis=1, keepdims=True), (WIDE, LANES))
        return c

    def weights(i, c):
        gi = sx * M + i - D
        ok = in_col & (gi >= 0) & (gi < GRID)
        here = KB[i + 1]
        kc = shifted(here)

        def pair(other, inside):
            both = ok & inside
            w = jnp.where(both, 2.0 * kc * other / jnp.where(both, kc + other, 1.0), 0.0)
            return w, jnp.where(ok & jnp.logical_not(inside), kc, w)
        edges = (pair(shifted(KB[i]), ok & (gi > 0)), pair(shifted(KB[i + 2]), ok & (gi < GRID - 1)),
                 pair(shifted(here, D - 1), gj > 0), pair(shifted(here, D + 1), gj < GRID - 1))
        total = 0.0
        for k, (w, d) in enumerate(edges):
            W5[k, i] = w
            total = total + d
        W5[SIDE, i] = total
        return c

    def pair_of(two, k):
        return jnp.concatenate(two, axis=0), pl.ds(mult(2 * ME * k), 2 * ME)

    def basis_rows(k, c):
        v, rows = pair_of([basis_of(shifted(S48[2, 2 * k + j])) for j in HALVES], k)
        put_middle(Ecat, rows, v)
        return c
    def geometry():
        up_down(k_v, "wait_send")
        up_down(k_in, "wait_recv")
        lax.fori_loop(0, M + 2 * OWN, kappa_rows, 0)
        lax.fori_loop(0, ME, weights, 0)
        for i in range(ME):
            RE[0, i:i + 1] = S48[2, i + 1, D - 1:D]
            RE[1, i:i + 1] = S48[2, i + 1, LOW:LOW + 1]
        lax.fori_loop(0, LOW // 2 - 1, basis_rows, 0)
        v, rows = pair_of([basis_of(RE[j]) for j in HALVES], LOW // 2 - 1)
        put_middle(Ecat, rows, v)

    def put_x(two, h, k):
        v, rows = pair_of(two, k)
        for j, piece in enumerate(split3(v)):
            X[j, rows, lanes(h)] = piece

    def put_rest():
        for slot, j in enumerate((0, 0, 1, 1, 2, 0)):
            Xr[REM * slot:REM * (slot + 1), :] = X[j, KM:NE, :]

    def first_rows(k, c):
        for h in HALVES:
            two = [shifted(S48[h, 2 * k + 1 + j]) for j in HALVES]
            for j in HALVES:
                Q[h, 2 * k + 1 + j] = two[j]
            put_x(two, h, k)
        return c
    lax.fori_loop(0, ME // 2, first_rows, 0)
    put_rest()

    colf = jnp.where((jcol >= D) & (jcol < D + M), 1.0, 0.0)
    sub8 = lax.broadcasted_iota(jnp.int32, (SUB, LANES), 0)
    zero = jnp.zeros((ME, LANES), F32)

    def product(start, n):
        first = NA
        outs = []
        for at, size in ((0, first), (first, n - first)):
            rows = pl.ds(mult(start + at), size)
            total = dot(Lr[rows, :], Xr[...])
            for j in PIECES:
                for i in PIECES[:len(PIECES) - j]:
                    total = total + dot(L[rows, KM * i:KM * (i + 1)], X[j, 0:KM, :])
            outs.append(total)
        return outs

    def put_t(outs, c):
        at = 0
        for v in outs:
            while v.shape[0]:
                top, off = 1 + ROWS * c + at // ME, at % ME
                n = min(ME - off, v.shape[0]) if off or v.shape[0] < ME else v.shape[0] // ME * ME
                whole = max(n // ME, 1)
                for h in HALVES:
                    T[h, pl.ds(top, whole), off:off + n // whole] = v[0:n, lanes(h)].reshape(whole, n // whole, LANES)
                v, at = v[n:], at + n

    def v_copy(e, par):
        return rc(T.at[:, pl.ds(1 + (M - 1) * e, STRIP)], V.at[par, 1 - e], v_s.at[e], v_r.at[par, 1 - e], {"sx": sx - 1 + 2 * e})

    def v_wait(e, par):
        v_copy(e, par).wait_send()
        rc(T.at[:, pl.ds(1, STRIP)], V.at[par, e], v_s.at[e], v_r.at[par, e], left).wait_recv()

    def step(m, carry):
        par = lax.rem(m, 2)

        def side(n, src, dst):
            return [rc(src[j], dst.at[par, 1 - j], hm_s.at[par, j, n], hm_r.at[par, 1 - j, n], (left, right)[j]) for j in HALVES]

        def cols(ref, lo, n):
            return [ref.at[:, pl.ds(lo, n), pl.ds(M * j, SUB)] for j in HALVES]

        mids = [side(n, cols(T, EDGE + ROWS * n, ROWS), HB.at[:, :, n]) for n in HALVES]
        edges = [side(2 + e, cols(TE, EDGE * e, EDGE), HE.at[:, :, e]) for e in (near, 1 - near)]
        parts = ((mult(BT * (1 - near)), ME - BT), (mult((ME - BT) * near, SUB), BT))
        rings = [side(SIDE + n, [PK.at[j, :, pl.ds(at, size)] for j in HALVES], HP.at[:, :, :, pl.ds(at, size)])
                 for n, (at, size) in enumerate(parts)]
        everything = mids + edges + rings
        v_near, v_far = v_copy(near, par), v_copy(1 - near, par)
        a2 = [rc(G1a, G2a.at[par, sx], a2_s.at[d - 1], a2_r.at[par, d - 1], {"sx": lax.rem(sx + d, SIDE)}) for d in FAR]

        def edge(e, pair):
            for h in HALVES:
                TE[h, pl.ds((EDGE + 2) * e, STRIP)] = T[h, pl.ds((M + 1) * e, STRIP)] + V[par, e, h]
                TE[h, pl.ds(STRIP + 2 * e, 2)] = T[h, pl.ds(STRIP + 2 * EDGE * e, 2)]
            go(pair)

        def ring_rows(pairs):
            for h in HALVES:
                for at, ref, k in pairs:
                    for j, lane in enumerate((SUB, M - 1)):
                        PK[j, h, at] = ref[h, k, lane:lane + 1]

        def ring_edge(e):
            for h in HALVES:
                for k in range(ROWS):
                    for j, lane in enumerate((SUB, M - 1)):
                        PK[j, h, pl.ds((M - 2) * e + k, 1)] = TE[h, pl.ds(ROWS * e + 1 + k, 1), lane:lane + 1].reshape(1, LANES)

        first = m == 0
        c_near, c_far = LAST * near, LAST * (1 - near)
        start = (LAST * CHUNK + BT) * near
        send_rows(Gd, d_s, d_r, [row(pqs[h], 0) for h in HALVES])
        out = product((LAST * CHUNK + BT) - start, CHUNK + BT)
        put_t([out[0][BT:], out[1]], c_far)
        for h in HALVES:
            G1a[mine_y, h] = out[0][0:SUB, lanes(h)][None]
        each(a1, "start")
        v_far.start()
        put_t(product(BT + start, CHUNK), c_near)
        pl.when(inner)(v_near.start)
        pl.when(jnp.logical_not(inner))(lambda: edge(near, edges[0]))
        v_wait(1 - near, par)
        edge(1 - near, edges[1])
        put_t(product(BT + CHUNK, CHUNK), 1)
        go(mids[0])
        each(a1, "wait")
        each(a2, "start")

        pq = full_sum(Gd, d_s, d_r)
        alpha = [jnp.where(first, -1.0, row(cst[0, h], 0) / row(pq, h)) for h in HALVES]

        tot = [[zero, zero] for h in HALVES]

        def update(c, inside):
            for h in HALVES:
                for k in range(ROWS):
                    i = 1 + ROWS * c + k
                    rn = r[h, i] - alpha[h] * Q[h, i]
                    ln = l[h, i] - alpha[h] * T[h, i]
                    r[h, i] = rn
                    l[h, i] = ln
                    x[h, i] = x[h, i] + alpha[h] * p[h, i]
                    w = colf if inside else jnp.where((i >= OWN) & (i < OWN + M), 1.0, 0.0) * colf
                    tot[h][0] = tot[h][0] + rn * ln
                    tot[h][1] = tot[h][1] + w * (rn * rn)

        out = product(BT + 2 * CHUNK, CHUNK)
        update(c_far, False)
        update(c_near, False)
        update(1, True)
        put_t(out, 2)
        update(2, True)
        G2a[par, mine_x] = G1a[...][None]
        each(a2, "wait_send")
        send_rows(Gb, b_s, b_r, [colsum(v) for two in tot for v in two])
        go(mids[1])
        ring_rows([(slice(i - 1, i), T, i) for i in range(EDGE, M - 1)])
        ring_edge(1 - near)
        go(rings[0])

        @pl.when(inner)
        def _():
            v_wait(near, par)
            edge(near, edges[0])
        ring_edge(near)
        go(rings[1])

        pl.when(first)(geometry)
        each(a2, "wait_recv")
        cq = jnp.concatenate([G2a[par, :, :, h].reshape(LANES, LANES) for h in HALVES], axis=1)
        yq = dot_pieces(lambda at: Ccat[:, at:at + TILE], cq)
        rzc = []
        for h in HALVES:
            cr[h] = cr[h] - alpha[h] * cq[:, lanes(h)]
            wr[h] = wr[h] - alpha[h] * yq[:, lanes(h)]
            rzc.append(colsum(cr[h] * wr[h]))
        n = LOW // 2
        for part in HALVES:
            o = dot_pieces(lambda at: Ecat[ME * n * part:ME * n * (part + 1), at:at + TILE], yq)
            for h in HALVES:
                Ey[h, n * part:n * (part + 1)] = o[:, lanes(h)].reshape(n, ME, LANES)

        got = full_sum(Gb, b_s, b_r)
        beta = []
        for h in HALVES:
            rzn = row(got, 2 * h) + rzc[h]
            rr = row(got, 2 * h + 1)
            beta.append(jnp.where(first, 0.0, rzn / row(cst[0, h], 0)))
            ff = jnp.where(first, jnp.sqrt(rr), row(cst[1, h], 0))
            cst[0, h] = wide(rzn)
            cst[1, h] = wide(ff)
            nrm_ref[:, lanes(h)] = jnp.where(sub8 == m - 1, jnp.sqrt(rr) / ff, nrm_ref[:, lanes(h)])

        def renew(i, u):
            for h in HALVES:
                zn = z[h, i] - alpha[h] * (u[h] + Ey[h, i])
                z[h, i] = zn
                p[h, i] = zn + beta[h] * p[h, i]

        def sides(b, buf, n, h, k):
            return jnp.concatenate([b[0:SUB] + buf[par, 0, n, h, k], b[SUB:M], b[M:] + buf[par, 1, n, h, k]], axis=0)

        def mid_rows(n):
            def body(k, c):
                i = EDGE + ROWS * n + k
                renew(i, [sides(T[h, i], HB, n, h, k) for h in HALVES])
                return c
            come(mids[n])
            lax.fori_loop(0, ROWS, body, 0)

        def edge_rows(e, pair):
            def body(k, c):
                renew((M - 1) * e + k, [sides(TE[h, EDGE * e + k], HE, e, h, k) for h in HALVES])
                return c
            come(pair)
            lax.fori_loop(0, EDGE, body, 0)

        def ring_cells(n):
            come(rings[n])
            at = pl.ds(*parts[n])
            for h in HALVES:
                for j in HALVES:
                    i = LOW - 2 + j
                    zn = z[h, i, at] - alpha[h] * (HP[par, j, h, at] + Ey[h, i, at])
                    z[h, i, at] = zn
                    p[h, i, at] = zn + beta[h] * p[h, i, at]

        def apply_rows(g, car):
            sums = list(car)
            rings = [[p[h, LOW - 2 + j, pl.ds(mult(SUB * g, SUB), SUB), :] for j in HALVES] for h in HALVES]
            rows = [[], []]
            for k in range(SUB):
                i = SUB * g + k
                w = [W5[j, i] for j in range(SIDE + 1)]
                own_f = jnp.where((i >= D) & (i < D + M), 1.0, 0.0) * colf
                for h in HALVES:
                    c = p[h, i + 1]
                    west = jnp.where(jcol == 0, row(rings[h][0], k), pltpu.roll(c, 1, 0))
                    east = jnp.where(jcol == ME - 1, row(rings[h][1], k), pltpu.roll(c, ME - 1, 0))
                    q = w[SIDE] * c
                    for j, other in enumerate((p[h, i], p[h, i + 2], west, east)):
                        q = q - w[j] * other
                    Q[h, i + 1] = q
                    sums[h] = sums[h] + own_f * (c * q)
                    rows[h].append(q)
                    if len(rows[h]) == 2:
                        put_x(rows[h], h, D * g + k // 2)
                        rows[h] = []
            return tuple(sums)
        edge_rows(1 - near, edges[1])
        mid_rows(0)
        mid_rows(1)
        ring_cells(0)
        low = 2 * (1 - near)
        car = lax.fori_loop(low, low + LAST, apply_rows, (zero, zero))
        edge_rows(near, edges[0])
        ring_cells(1)
        low = LAST * near
        car = lax.fori_loop(low, low + 2, apply_rows, car)
        put_rest()
        for h in HALVES:
            pqs[h] = wide(colsum(car[h]))

        for pair in everything:
            gone(pair)
        return carry

    lax.fori_loop(0, ITERS, step, 0)

    send_rows(Gd, d_s, d_r, [row(pqs[h], 0) for h in HALVES])
    pq = full_sum(Gd, d_s, d_r)
    alpha = [row(cst[0, h], 0) / row(pq, h) for h in HALVES]

    def finish(i, car):
        res = []
        for h in HALVES:
            rn = r[h, i] - alpha[h] * Q[h, i]
            res.append(car[h] + colf * (rn * rn))
            xn = x[h, i] + alpha[h] * p[h, i]
            T[h, i, 0:M] = pltpu.roll(jnp.concatenate([xn, xn[0:SUB]], axis=0), WIDE - D, 0)[0:M]
        return tuple(res)
    rr = lax.fori_loop(OWN, OWN + M, finish, (zero, zero))
    out_cp = [pltpu.make_async_copy(T.at[h, own, pl.ds(0, M)], x_hbm.at[:, :, pl.ds(LANES * h, LANES)], out_sem.at[h]) for h in HALVES]
    each(out_cp, "start")
    send_rows(Gb, b_s, b_r, [colsum(v) for v in rr])
    got = full_sum(Gb, b_s, b_r)
    for h in HALVES:
        nrm_ref[:, lanes(h)] = jnp.where(sub8 == ITERS - 1, jnp.sqrt(row(got, h)) / row(cst[1, h], 0), nrm_ref[:, lanes(h)])
    each(out_cp, "wait")


def solution(mesh):
    def dma(*shape):
        return pltpu.SemaphoreType.DMA(shape)

    def vm(*shape, dtype=F32):
        return pltpu.VMEM(shape, dtype)

    field = vm(2, LOW, ME, LANES)
    strips = [vm(2, 2, 2, 2, n, SUB, LANES) for n in (ROWS, EDGE)]
    gathers = [vm(SIDE, 2, SUB, LANES), vm(2, SIDE, SIDE, 2, SUB, LANES)] + [vm(SIDE * SIDE, SIDE, LANES)] * 2
    scratch = [
        vm(len(PIECES), M + 2 * OWN, WIDE, LANES), vm(NL, KM * len(PIECES), dtype=BF16), vm(NL, 2 * TILE, dtype=BF16),
        vm(SIDE, CHUNK, NE), vm(len(PIECES), NE, TILE, dtype=BF16), vm(2 * TILE, TILE, dtype=BF16),
        field, vm(2, 2 * EDGE, ME, LANES), field, field, field, field, field, field, field,
        vm(SIDE + 1, ME, ME, LANES), vm(LOW * ME, LANES * len(PIECES), dtype=BF16), vm(2, ME, LANES), vm(M + 2 * OWN, WIDE, LANES), vm(LANES, NP),
        *[vm(2, 2, M // 2, SUB, LANES)] * 2,
        vm(2, 2, 2, STRIP, ME, LANES), *strips, vm(2, 2, 2, ME, LANES), vm(2, 2, ME, LANES), *gathers,
        vm(LANES, LANES * len(PIECES), dtype=BF16), vm(2, LANES, LANES), vm(2, LANES, LANES), vm(2, 2, SUB, LANES),
        vm(2, SUB, LANES), dma(SIDE), dma(2), *[dma(2)] * 9, dma(2, 2), *[dma(2, 2, SIDE + 2)] * 2,
        *[dma(LAST)] * 3, dma(2, LAST), *[dma(SIDE * SIDE - 1)] * 4, dma(2),
    ]
    any_spec = pl.BlockSpec(memory_space=pl.ANY)
    vmem_spec = pl.BlockSpec(memory_space=pltpu.VMEM)

    def body(forcing, kappa, local_inv, coarse_basis, coarse_counts, coarse_inv):
        index = lax.axis_index("sx") * SIDE + lax.axis_index("sy")
        own = jnp.concatenate([coarse_basis[0].T[:KMAX - 1], kappa.reshape(1, M * M)], axis=0)
        mine = jnp.arange(LANES) // KMAX == index
        cnt = jnp.broadcast_to(jnp.where(mine, coarse_counts.astype(F32), 0.0)[None, :], (SUB, LANES))
        return pl.pallas_call(
            solve_kernel,
            out_shape=(jax.ShapeDtypeStruct((M, M, 2 * LANES), F32), jax.ShapeDtypeStruct((ITERS, 2 * LANES), F32)),
            in_specs=[any_spec] * 2 + [vmem_spec] * len(PIECES),
            out_specs=(any_spec, vmem_spec),
            scratch_shapes=scratch,
            compiler_params=pltpu.CompilerParams(collective_id=0, has_side_effects=True, vmem_limit_bytes=67043328),
        )(forcing, local_inv[0], own, coarse_inv, cnt)

    cell_spec = P(("batch", "sx"), "sy", None)
    sub_spec = P(("batch", "sx", "sy"), None, None)
    return jax.shard_map(body, mesh=mesh, in_specs=(cell_spec, P(("batch", "sx"), "sy"), sub_spec, sub_spec, P(("batch", "sx", "sy")), P("batch", None)), out_specs=(cell_spec, P("batch", None)), check_vma=False)
```
